32 devices in a mesh: freq: 32 (over z, y, x, core).
Axes of the slice: x: 2, y: 2, z: 4, core: 2. Of those that a mesh axis runs over, the one named last changes fastest.
Arguments:
- pulses: float32 [1, 2, 30, 65536], P(None, None, None, 'freq'), may hold values from -4 to 4
- coupling: float32 [2, 30, 30, 65536], P(None, None, None, 'freq'), may hold values from -0.4 to 0.4
- dispersion_terms: float32 [3, 30], replicated, may hold values from -3 to 3
- kerr_gain: float32 [30], replicated, may hold values from 0.01 to 0.08
Outputs:
- evolved: float32 [1, 2, 30, 65536], P(None, None, None, 'freq')
The draws below stay inside these ranges and needn't reach their ends.
All inputs are finite; a program needn't handle non-finite values.
Results may differ from the reference program's by a relative error of at most 0.00027.
Values sent between devices are 32-bit elements; how exact they have to be, the bound alone decides.
A program may use at most 128 MiB of HBM per device.

```python
import math
import jax
import jax.numpy as jnp
from jax import lax

M = 30
TPTS = 65536
STEPS = 2
PULSES = 1
FLOC = 2048
N_FREQ = 32


def steps_of(key, shape, cuts, smallest, top_value):
    def one(dim, shards_of):
        draws = jax.random.uniform(jax.random.fold_in(jax.random.fold_in(key, 6), dim), (shards_of,), jnp.float32, smallest / len(cuts), top_value / len(cuts))
        return jnp.repeat(jnp.exp(draws), shape[dim] // shards_of).reshape((-1,) + (1,) * (len(shape) - dim - 1))

    gain = one(*cuts[0])
    for cut in cuts[1:]:
        gain = gain * one(*cut)
    return gain


def noise(key, shape, spread, bound, split=(), kind=jnp.bfloat16):
    gain = steps_of(key, shape, split, -0.22, 0.18) if split else 1.0
    entries = jax.random.normal(key, shape, jnp.float32) * spread * gain
    return jnp.minimum(jnp.maximum(entries, -bound), bound).astype(kind)


def setup_inputs(seed: int = 0) -> dict:
    key_list = jax.random.split(jax.random.key(seed), 5)
    return {
        "pulses": noise(key_list[0], (PULSES, 2, M, TPTS), 0.5, 4.0, ((3, 32),), jnp.float32),
        "coupling": noise(key_list[1], (2, M, M, TPTS), 0.06, 0.4, ((3, 32),), jnp.float32),
        "dispersion_terms": jnp.clip(jax.random.uniform(key_list[2], (3, M), jnp.float32, -3.0, 3.0), -3.0, 3.0),
        "kerr_gain": jnp.clip(jnp.exp(jax.random.uniform(key_list[3], (M,), jnp.float32, math.log(0.01), math.log(0.08))), 0.01, 0.08),
    }


def reference(pulses, coupling, dispersion_terms, kerr_gain):
    complex_field = pulses[:, 0] + 1j * pulses[:, 1]
    bin_order = coupling.reshape(2, M, M, N_FREQ, FLOC).transpose(0, 1, 2, 4, 3).reshape(2, M, M, TPTS)
    identity = jnp.eye(M, dtype=jnp.float32)[:, :, None]
    mixing = (bin_order[0] + identity) + 1j * bin_order[1]
    bin_index = jnp.arange(TPTS, dtype=jnp.int32)
    signed_bin = jnp.where(bin_index < TPTS // 2, bin_index, bin_index - TPTS).astype(jnp.float32)
    angular = signed_bin / (TPTS // 2)
    dispersion = (dispersion_terms[0][:, None] * angular + dispersion_terms[1][:, None] * angular ** 2 / 2
                  + dispersion_terms[2][:, None] * angular ** 3 / 6)
    rotation = jnp.cos(dispersion) + 1j * jnp.sin(dispersion)
    for repeat in range(STEPS):
        spectrum = jnp.fft.fft(complex_field, axis=-1)
        spectrum = jnp.einsum("nmk,bmk->bnk", mixing, spectrum, precision=lax.Precision.HIGHEST)
        spectrum = spectrum * rotation
        complex_field = jnp.fft.ifft(spectrum, axis=-1)
        magnitude = jnp.real(complex_field) ** 2 + jnp.imag(complex_field) ** 2
        total_power = jnp.sum(magnitude, axis=1, keepdims=True)
        nonlinear = kerr_gain[None, :, None] * (2.0 * total_power - magnitude)
        complex_field = complex_field * (jnp.cos(nonlinear) + 1j * jnp.sin(nonlinear))
    return jnp.stack((jnp.real(complex_field), jnp.imag(complex_field)), axis=1).astype(jnp.float32)
```

```python
import functools

import jax
import jax.numpy as jnp
import numpy as np
from jax import lax
from jax.experimental import pallas as pl
from jax.experimental.pallas import tpu as pltpu
from jax.sharding import PartitionSpec as P

STEPS = 2


HIGHEST = lax.Precision.HIGHEST


def angle_table(first, second, modulus, orient):
    turns = first[:, None] * second[None, :] % modulus
    radians = turns.astype(jnp.float32) * (2.0 * jnp.pi / modulus)
    return (jnp.cos(radians), orient * jnp.sin(radians))


def rotate(real_part, imag_part, cosine, sine):
    return (real_part * cosine - imag_part * sine, real_part * sine + imag_part * cosine)


def transform(stacked, cosine, sine):
    real_part = stacked[:, 0]
    imag_part = stacked[:, 1]
    out_real = jnp.matmul(real_part, cosine, precision=HIGHEST) - jnp.matmul(
        imag_part, sine, precision=HIGHEST
    )
    out_imag = jnp.matmul(real_part, sine, precision=HIGHEST) + jnp.matmul(
        imag_part, cosine, precision=HIGHEST
    )
    return jnp.stack((out_real, out_imag), axis=1)


def nonlinear_phase(stacked, kerr_gain):
    magnitude = stacked[:, 0] ** 2 + stacked[:, 1] ** 2
    total_power = jnp.sum(magnitude, axis=1, keepdims=True)
    gains = kerr_gain.reshape((1, -1) + (1,) * (magnitude.ndim - 2))
    angles = gains * (2.0 * total_power - magnitude)
    real_part, imag_part = rotate(stacked[:, 0], stacked[:, 1], jnp.cos(angles), jnp.sin(angles))
    return jnp.stack((real_part, imag_part), axis=1)


def per_device(pulses, coupling, dispersion_terms, kerr_gain):
    shards = lax.axis_size("freq")
    device = lax.axis_index("freq")
    mode_count = pulses.shape[2]
    local_count = pulses.shape[3]
    groups = local_count // shards
    total_count = local_count * shards
    column_index = jnp.arange(shards, dtype=jnp.int32)
    row_index = jnp.arange(local_count, dtype=jnp.int32)
    short_cos, short_sin = angle_table(column_index, column_index, shards, -1.0)
    inverse_short_cos, inverse_short_sin = angle_table(column_index, column_index, shards, 1.0)
    long_cos, long_sin = angle_table(row_index, row_index, local_count, -1.0)
    inverse_long_cos, inverse_long_sin = angle_table(row_index, row_index, local_count, 1.0)
    sample_rows = jnp.arange(groups, dtype=jnp.int32) * shards + device
    twist_cos, twist_sin = angle_table(sample_rows, column_index, total_count, -1.0)
    untwist_cos, untwist_sin = angle_table(row_index, jnp.reshape(device, (1,)), total_count, 1.0)
    untwist_cos = untwist_cos.reshape(-1)
    untwist_sin = untwist_sin.reshape(-1)
    bins = device + shards * row_index
    signed_bin = jnp.where(bins < total_count // 2, bins, bins - total_count).astype(jnp.float32)
    angular = signed_bin / (total_count // 2)
    dispersion = (
        dispersion_terms[0][:, None] * angular
        + dispersion_terms[1][:, None] * angular**2 / 2
        + dispersion_terms[2][:, None] * angular**3 / 6
    )
    spread_cos = jnp.cos(dispersion)
    spread_sin = jnp.sin(dispersion)
    identity = jnp.eye(mode_count, dtype=jnp.float32)[:, :, None]
    mixing_real = coupling[0] + identity
    mixing_imag = coupling[1]
    blocks = pulses.reshape(pulses.shape[0], 2, mode_count, groups, shards)
    columns = lax.all_to_all(blocks, "freq", split_axis=4, concat_axis=4, tiled=True)
    for repeat in range(STEPS):
        spectral = transform(columns, short_cos, short_sin)
        forward_real_part, forward_imag_part = rotate(
            spectral[:, 0], spectral[:, 1], twist_cos, twist_sin
        )
        evolve_rows = lax.all_to_all(
            jnp.stack((forward_real_part, forward_imag_part), axis=1),
            "freq",
            split_axis=4,
            concat_axis=4,
            tiled=True,
        )
        flat = evolve_rows.reshape(evolve_rows.shape[0], 2, mode_count, local_count)
        spectrum = transform(flat, long_cos, long_sin)
        spec_real = spectrum[:, 0]
        spec_imag = spectrum[:, 1]
        mixed_real = jnp.einsum(
            "nmk,bmk->bnk", mixing_real, spec_real, precision=HIGHEST
        ) - jnp.einsum("nmk,bmk->bnk", mixing_imag, spec_imag, precision=HIGHEST)
        mixed_imag = jnp.einsum(
            "nmk,bmk->bnk", mixing_real, spec_imag, precision=HIGHEST
        ) + jnp.einsum("nmk,bmk->bnk", mixing_imag, spec_real, precision=HIGHEST)
        real_part, imag_part = rotate(mixed_real, mixed_imag, spread_cos, spread_sin)
        inverted = transform(
            jnp.stack((real_part, imag_part), axis=1), inverse_long_cos, inverse_long_sin
        )
        real_part, imag_part = rotate(inverted[:, 0], inverted[:, 1], untwist_cos, untwist_sin)
        moved = jnp.stack((real_part, imag_part), axis=1).reshape(evolve_rows.shape)
        columns = nonlinear_phase(
            transform(
                lax.all_to_all(moved, "freq", split_axis=4, concat_axis=4, tiled=True),
                inverse_short_cos,
                inverse_short_sin,
            )
            * (1.0 / total_count),
            kerr_gain,
        )
    returned = lax.all_to_all(columns, "freq", split_axis=4, concat_axis=4, tiled=True)
    return returned.reshape(columns.shape[0], 2, mode_count, local_count)


LANES = 128
HALF = LANES // 2
SUB = 8


def low_lanes(shape):
    return lax.broadcasted_iota(jnp.int32, shape, len(shape) - 1) < HALF


def swap(x):
    return pltpu.roll(x, HALF, 1)


def sign_row(rows):
    return jnp.where(low_lanes((rows, LANES)), -1.0, 1.0).astype(jnp.float32)


def times_root(x, index, count, orient, sgn):
    eighth = 8 * index
    if index == 0:
        return x
    if eighth == 2 * count:
        return swap(x) * (sgn * orient)
    angle = 2.0 * np.pi * index / count
    return x * float(np.cos(angle)) + swap(x) * (sgn * float(orient * np.sin(angle)))


def short_fft(items, orient, sgn):
    count = len(items)
    if count == 1:
        return items
    even = short_fft(items[0::2], orient, sgn)
    odd = short_fft(items[1::2], orient, sgn)
    turned = [times_root(v, k, count, orient, sgn) for k, v in enumerate(odd)]
    return [e + t for e, t in zip(even, turned)] + [e - t for e, t in zip(even, turned)]


def packed_mul(x, cosine, signed_sine):
    return x * cosine + swap(x) * signed_sine


def split_constant(value, pieces, bits):
    parts = []
    for _ in range(pieces - 1):
        exponent = np.floor(np.log2(value))
        unit = 2.0 ** (exponent - bits + 1)
        part = np.floor(value / unit) * unit
        parts.append(float(part))
        value -= part
    return parts + [float(value)]


HALF_PI = split_constant(np.pi / 2, 4, 8)


def sine_cosine(theta):
    turns = jnp.floor(theta * float(2 / np.pi) + 0.5)
    rest = theta
    for part in HALF_PI:
        rest = rest - turns * part
    square = rest * rest
    sine = rest + rest * square * (
        -1.6666654611e-1 + square * (8.3321608736e-3 - square * 1.9515295891e-4)
    )
    cosine = 1.0 - 0.5 * square + square * square * (
        4.166664568298827e-2 + square * (-1.388731625493765e-3 + square * 2.443315711809948e-5)
    )
    quadrant = turns.astype(jnp.int32) & 3
    crossed = (quadrant & 1) == 1
    out_sine = jnp.where(crossed, cosine, sine)
    out_cosine = jnp.where(crossed, sine, cosine)
    out_sine = jnp.where(quadrant >= 2, -out_sine, out_sine)
    out_cosine = jnp.where((quadrant == 1) | (quadrant == 2), -out_cosine, out_cosine)
    return out_sine, out_cosine


def long_dft(x, weights):
    high = x.astype(jnp.bfloat16)
    low = (x - high.astype(jnp.float32)).astype(jnp.bfloat16)
    both = jnp.concatenate((high, low), axis=1)
    product = jnp.dot(both, weights, preferred_element_type=jnp.float32)
    return product[:, :LANES] + product[:, LANES:]


def mega_kernel(
    count, modes, scale, x_ref, c_hbm, spread_cos_ref, spread_sin_ref, tw_cos_ref, tw_sin_ref,
    twist_cos_ref, twist_sin_ref, gain_ref, fwd_ref, inv_ref, out_ref,
    c_ref, recv, send, spec, by_real, by_imag, total, field, acc, send_sem, recv_sem, c_sem,
):
    me = lax.axis_index("freq")
    rows = x_ref.shape[1]
    chunks = rows // SUB
    last = modes - (chunks - 1) * SUB
    width = c_ref.shape[2]
    pitch = by_real.shape[0] // rows
    sgn = sign_row(SUB)
    low = low_lanes((SUB, LANES))
    odd = lax.broadcasted_iota(jnp.int32, (SUB, LANES), 0) % 2 == 1
    exchanges = recv.shape[0]

    def tile_rows(c):
        return pl.ds(pl.multiple_of(c * SUB, SUB), SUB)

    def by_size(c, fn):
        if last == SUB:
            fn(SUB)
        else:
            pl.when(c < chunks - 1)(lambda: fn(SUB))
            pl.when(c == chunks - 1)(lambda: fn(last))

    def remote(src, dst, ex, c, peer):
        return pltpu.make_async_remote_copy(
            src_ref=src,
            dst_ref=dst,
            send_sem=send_sem.at[ex],
            recv_sem=recv_sem.at[ex, c],
            device_id=(peer,),
            device_id_type=pl.DeviceIdType.MESH,
        )

    def post(src, ex, c):
        def sized(size):
            at = pl.ds(pl.multiple_of(c * SUB, SUB), size)
            recv[ex, me, at, :] = src[me, at, :]

            def one(j, carry):
                peer = (me + count // 2 + (j // 2) * (1 - 2 * (j % 2))) % count
                remote(src.at[peer, at], recv.at[ex, me, at], ex, c, peer).start()
                return carry

            lax.fori_loop(1, count, one, 0)

        by_size(c, sized)

    def arrive(ex, c):
        def sized(size):
            at = pl.ds(pl.multiple_of(c * SUB, SUB), size)
            part = recv.at[ex, pl.ds(0, count - 1), at]
            remote(part, part, ex, c, (me + 1) % count).wait_recv()

        by_size(c, sized)

    def each(body):
        def step(c, carry):
            body(c)
            return carry

        lax.fori_loop(0, chunks, step, 0)

    if rows > modes:
        spare = pl.ds(modes, rows - modes)
        for ex in range(exchanges):
            recv[ex, :, spare, :] = jnp.zeros((count, rows - modes, LANES), jnp.float32)
    total[...] = jnp.zeros_like(total)

    load = pltpu.make_async_copy(c_hbm, c_ref, c_sem)
    load.start()
    barrier = pltpu.get_barrier_semaphore()

    def greet(k, carry):
        pl.semaphore_signal(
            barrier, inc=1, device_id=((me + k) % count,), device_id_type=pl.DeviceIdType.MESH
        )
        return carry

    lax.fori_loop(1, count, greet, 0)
    pl.semaphore_wait(barrier, count - 1)

    each(lambda c: post(x_ref, 0, c))

    def columns_out(source, dst, ex, c):
        at = tile_rows(c)
        items = short_fft([source[a, at, :] for a in range(count)], -1.0, sgn)
        for d, value in enumerate(items):
            dst[d, at, :] = packed_mul(value, twist_cos_ref[d : d + 1, :], twist_sin_ref[d : d + 1, :])
        post(dst, ex, c)

    def row_in(ex, c):
        at = tile_rows(c)
        block = recv[ex, :, at, :].reshape(count * SUB, LANES)
        spec[...] = long_dft(block, fwd_ref[...]).reshape(count, SUB, LANES)
        items = short_fft(
            [
                packed_mul(spec[p], tw_cos_ref[p : p + 1, :], tw_sin_ref[p : p + 1, :])
                for p in range(count)
            ],
            -1.0,
            sgn,
        )
        for tile in range(width // 2):
            first, second = items[2 * tile], items[2 * tile + 1]
            real = jnp.where(low, first, swap(second))
            imag = jnp.where(low, swap(first), second)
            for part in range(2):
                to = pl.ds(c * SUB * pitch + 2 * tile + part, SUB, stride=pitch)
                by_real[to, :] = real
                by_imag[to, :] = imag

    def mix(c, size):
        def body(q, carry):
            def spot(index):
                return pl.ds(pl.multiple_of(index * pitch + q * SUB, SUB), SUB)

            with_real = [
                jnp.where(odd, by_imag[spot(c * SUB + g), :], by_real[spot(c * SUB + g), :])
                for g in range(size)
            ]
            with_imag = [jnp.zeros((SUB, LANES), jnp.float32) for _ in range(size)]
            for m in range(modes):
                real, imag = by_real[spot(m), :], by_imag[spot(m), :]
                for g in range(size):
                    factor = c_ref[c * SUB + g, m, tile_rows(q), :]
                    with_real[g] = with_real[g] + factor * real
                    with_imag[g] = with_imag[g] + factor * imag
            for g in range(size):
                other = jnp.where(
                    odd, pltpu.roll(with_imag[g], 1, 0), -pltpu.roll(with_imag[g], SUB - 1, 0)
                )
                total[spot(g), :] = with_real[g] + other
            return carry

        lax.fori_loop(0, width // SUB, body, 0)

    def row_out(dst, ex, c):
        at = tile_rows(c)
        by_size(c, lambda size: mix(c, size))
        items = []
        for tile in range(width // 2):
            lanes = pl.ds(tile * LANES, LANES)
            real, imag = rotate(
                total[pl.ds(2 * tile, SUB, stride=pitch), :],
                total[pl.ds(2 * tile + 1, SUB, stride=pitch), :],
                spread_cos_ref[at, lanes],
                spread_sin_ref[at, lanes],
            )
            items.append(jnp.where(low, real, swap(imag)))
            items.append(jnp.where(low, swap(real), imag))
        for p, value in enumerate(short_fft(items, 1.0, sgn)):
            spec[p] = packed_mul(value, tw_cos_ref[p : p + 1, :], -tw_sin_ref[p : p + 1, :])
        block = spec[...].reshape(count * SUB, LANES)
        dst[:, at, :] = long_dft(block, inv_ref[...]).reshape(count, SUB, LANES)
        post(dst, ex, c)

    def columns_in(ex, c):
        at = tile_rows(c)
        items = [
            packed_mul(
                recv[ex, d, at, :],
                twist_cos_ref[d : d + 1, :] * scale,
                twist_sin_ref[d : d + 1, :] * -scale,
            )
            for d in range(count)
        ]
        for a, value in enumerate(short_fft(items, 1.0, sgn)):
            field[a, at, :] = value
            acc[a] = acc[a] + value * value

    def power():
        def body(a, carry):
            part = jnp.sum(acc[a], axis=0, keepdims=True)
            acc[a] = jnp.broadcast_to(2.0 * (part + swap(part)), (SUB, LANES))
            return carry

        lax.fori_loop(0, count, body, 0, unroll=4)

    def kerr(target, c):
        at = tile_rows(c)
        gain = gain_ref[at, :]

        def body(a, carry):
            x = field[a, at, :]
            square = x * x
            magnitude = square + swap(square)
            sine, cosine = sine_cosine(gain * (acc[a] - magnitude))
            target[a, at, :] = packed_mul(x, cosine, sine * sgn)
            return carry

        lax.fori_loop(0, count, body, 0, unroll=4)

    ex = 1
    for repeat in range(STEPS):
        dst = send.at[ex - 1]
        if repeat == 0:

            def begin(c):
                arrive(0, c)
                columns_out(recv.at[0], dst, ex, c)

            each(begin)
        else:
            power()

            def bend(c):
                kerr(field, c)
                columns_out(field, dst, ex, c)

            each(bend)

        def inward(c):
            arrive(ex, c)
            row_in(ex, c)

        each(inward)
        if repeat == 0:
            load.wait()
        ex += 1
        each(lambda c: row_out(send.at[ex - 1], ex, c))
        acc[...] = jnp.zeros_like(acc)

        def collect(c):
            arrive(ex, c)
            columns_in(ex, c)

        each(collect)
        ex += 1
    power()

    def finish(c):
        kerr(send.at[ex - 1], c)
        post(send.at[ex - 1], ex, c)

    each(finish)

    def result(c):
        arrive(ex, c)
        out_ref[:, tile_rows(c), :] = recv[ex, :, tile_rows(c), :]

    each(result)
    for ex in range(exchanges):
        sent = recv.at[ex, pl.ds(0, count - 1), pl.ds(0, modes)]
        remote(sent, sent, ex, 0, (me + 1) % count).wait_send()


def mega(x, coupling, spread_cos, spread_sin, tw_cos, tw_sin, twist_cos, twist_sin, gain, fwd, inv, modes, scale):
    count, rows = x.shape[0], x.shape[1]
    width = coupling.shape[2]
    pitch = width + SUB
    exchanges = 2 * STEPS + 2
    chunks = rows // SUB
    vmem = pl.BlockSpec(memory_space=pltpu.VMEM)
    block = (count, rows, LANES)
    return pl.pallas_call(
        functools.partial(mega_kernel, count, modes, scale),
        out_shape=jax.ShapeDtypeStruct(x.shape, x.dtype),
        in_specs=[vmem, pl.BlockSpec(memory_space=pl.ANY)] + [vmem] * 9,
        out_specs=vmem,
        scratch_shapes=[
            pltpu.VMEM(coupling.shape, jnp.float32),
            pltpu.VMEM((exchanges,) + block, jnp.float32),
            pltpu.VMEM((exchanges - 1,) + block, jnp.float32),
            pltpu.VMEM((count, SUB, LANES), jnp.float32),
            pltpu.VMEM((rows * pitch, LANES), jnp.float32),
            pltpu.VMEM((rows * pitch, LANES), jnp.float32),
            pltpu.VMEM((SUB * pitch, LANES), jnp.float32),
            pltpu.VMEM(block, jnp.float32),
            pltpu.VMEM((count, SUB, LANES), jnp.float32),
            pltpu.SemaphoreType.DMA((exchanges,)),
            pltpu.SemaphoreType.DMA((exchanges, chunks)),
            pltpu.SemaphoreType.DMA(()),
        ],
        compiler_params=pltpu.CompilerParams(collective_id=0, has_side_effects=True),
        name="mega",
    )(x, coupling, spread_cos, spread_sin, tw_cos, tw_sin, twist_cos, twist_sin, gain, fwd, inv)


def packed_table(cosine, sine):
    xp = np if isinstance(cosine, np.ndarray) else jnp
    return (
        xp.concatenate((cosine, cosine), axis=1).astype(xp.float32),
        xp.concatenate((-sine, sine), axis=1).astype(xp.float32),
    )


def dft_weights(size, orient):
    index = np.arange(size)
    angle = orient * 2.0 * np.pi * (index[:, None] * index[None, :] % size) / size
    cosine, sine = np.cos(angle), np.sin(angle)
    full = np.block([[cosine, sine], [-sine, cosine]]).astype(np.float32)
    high = full.astype(jnp.bfloat16)
    low = (full - high.astype(np.float32)).astype(jnp.bfloat16)
    return np.block([[high, low], [high, np.zeros_like(low)]])


def packed_device(pulses, coupling, dispersion_terms, kerr_gain):
    shards = lax.axis_size("freq")
    device = lax.axis_index("freq")
    modes, local = pulses.shape[2], pulses.shape[3]
    groups = local // shards
    total = local * shards
    rows = -(-modes // SUB) * SUB
    pad = rows - modes

    shard_index = np.arange(shards)
    angle = -2.0 * np.pi * (shard_index[:, None] * np.arange(groups)[None, :] % local) / local
    tw_cos, tw_sin = packed_table(np.cos(angle), np.sin(angle))
    fwd, inv = dft_weights(groups, -1.0), dft_weights(groups, 1.0)
    samples = device + shards * jnp.arange(groups, dtype=jnp.int32)
    twist_cos, twist_sin = packed_table(
        *angle_table(jnp.arange(shards, dtype=jnp.int32), samples, total, -1.0)
    )
    gain = jnp.broadcast_to(jnp.pad(kerr_gain, (0, pad))[:, None], (rows, LANES))

    bins = device + shards * jnp.arange(local, dtype=jnp.int32)
    signed_bin = jnp.where(bins < total // 2, bins, bins - total).astype(jnp.float32)
    angular = signed_bin / (total // 2)
    terms = jnp.pad(dispersion_terms, ((0, 0), (0, pad)))
    dispersion = (
        terms[0][:, None] * angular
        + terms[1][:, None] * angular**2 / 2
        + terms[2][:, None] * angular**3 / 6
    )
    spread_cos, spread_sin = jnp.cos(dispersion), jnp.sin(dispersion)

    coupling = coupling.reshape(2, modes, modes, local // LANES, LANES).transpose(1, 2, 3, 0, 4)
    coupling = coupling.reshape(modes, modes, 2 * local // LANES, LANES)
    blocks = pulses.reshape(2, modes, groups, shards).transpose(3, 1, 0, 2)
    x = jnp.pad(blocks.reshape(shards, modes, 2 * groups), ((0, 0), (0, pad), (0, 0)))
    scale = 1.0 / total
    x = mega(
        x, coupling, spread_cos, spread_sin, tw_cos, tw_sin, twist_cos, twist_sin, gain, fwd, inv, modes, scale
    )
    x = x[:, :modes].reshape(shards, modes, 2, groups).transpose(2, 1, 3, 0)
    return x.reshape(1, 2, modes, local)


def fits(shards, pulses):
    local = pulses.shape[3] // shards
    return (
        pulses.shape[0] == 1
        and shards & (shards - 1) == 0
        and shards >= 4
        and local == shards * HALF
    )


def solution(mesh):
    in_specs = (P(None, None, None, "freq"), P(None, None, None, "freq"), P(), P())
    out_specs = P(None, None, None, "freq")
    shards = mesh.shape["freq"]

    def run(pulses, coupling, dispersion_terms, kerr_gain):
        body = packed_device if fits(shards, pulses) else per_device
        return jax.shard_map(
            body, mesh=mesh, in_specs=in_specs, out_specs=out_specs, check_vma=False
        )(pulses, coupling, dispersion_terms, kerr_gain)

    return run
```

```python
import functools

import jax
import jax.numpy as jnp
import numpy as np
from jax import lax
from jax.experimental import pallas as pl
from jax.experimental.pallas import tpu as pltpu
from jax.sharding import PartitionSpec as P

STEPS = 2


HIGHEST = lax.Precision.HIGHEST


def angle_table(first, second, modulus, orient):
    turns = first[:, None] * second[None, :] % modulus
    radians = turns.astype(jnp.float32) * (2.0 * jnp.pi / modulus)
    return (jnp.cos(radians), orient * jnp.sin(radians))


def rotate(real_part, imag_part, cosine, sine):
    return (real_part * cosine - imag_part * sine, real_part * sine + imag_part * cosine)


def transform(stacked, cosine, sine):
    real_part = stacked[:, 0]
    imag_part = stacked[:, 1]
    out_real = jnp.matmul(real_part, cosine, precision=HIGHEST) - jnp.matmul(
        imag_part, sine, precision=HIGHEST
    )
    out_imag = jnp.matmul(real_part, sine, precision=HIGHEST) + jnp.matmul(
        imag_part, cosine, precision=HIGHEST
    )
    return jnp.stack((out_real, out_imag), axis=1)


def nonlinear_phase(stacked, kerr_gain):
    magnitude = stacked[:, 0] ** 2 + stacked[:, 1] ** 2
    total_power = jnp.sum(magnitude, axis=1, keepdims=True)
    gains = kerr_gain.reshape((1, -1) + (1,) * (magnitude.ndim - 2))
    angles = gains * (2.0 * total_power - magnitude)
    real_part, imag_part = rotate(stacked[:, 0], stacked[:, 1], jnp.cos(angles), jnp.sin(angles))
    return jnp.stack((real_part, imag_part), axis=1)


def per_device(pulses, coupling, dispersion_terms, kerr_gain):
    shards = lax.axis_size("freq")
    device = lax.axis_index("freq")
    mode_count = pulses.shape[2]
    local_count = pulses.shape[3]
    groups = local_count // shards
    total_count = local_count * shards
    column_index = jnp.arange(shards, dtype=jnp.int32)
    row_index = jnp.arange(local_count, dtype=jnp.int32)
    short_cos, short_sin = angle_table(column_index, column_index, shards, -1.0)
    inverse_short_cos, inverse_short_sin = angle_table(column_index, column_index, shards, 1.0)
    long_cos, long_sin = angle_table(row_index, row_index, local_count, -1.0)
    inverse_long_cos, inverse_long_sin = angle_table(row_index, row_index, local_count, 1.0)
    sample_rows = jnp.arange(groups, dtype=jnp.int32) * shards + device
    twist_cos, twist_sin = angle_table(sample_rows, column_index, total_count, -1.0)
    untwist_cos, untwist_sin = angle_table(row_index, jnp.reshape(device, (1,)), total_count, 1.0)
    untwist_cos = untwist_cos.reshape(-1)
    untwist_sin = untwist_sin.reshape(-1)
    bins = device + shards * row_index
    signed_bin = jnp.where(bins < total_count // 2, bins, bins - total_count).astype(jnp.float32)
    angular = signed_bin / (total_count // 2)
    dispersion = (
        dispersion_terms[0][:, None] * angular
        + dispersion_terms[1][:, None] * angular**2 / 2
        + dispersion_terms[2][:, None] * angular**3 / 6
    )
    spread_cos = jnp.cos(dispersion)
    spread_sin = jnp.sin(dispersion)
    identity = jnp.eye(mode_count, dtype=jnp.float32)[:, :, None]
    mixing_real = coupling[0] + identity
    mixing_imag = coupling[1]
    blocks = pulses.reshape(pulses.shape[0], 2, mode_count, groups, shards)
    columns = lax.all_to_all(blocks, "freq", split_axis=4, concat_axis=4, tiled=True)
    for repeat in range(STEPS):
        spectral = transform(columns, short_cos, short_sin)
        forward_real_part, forward_imag_part = rotate(
            spectral[:, 0], spectral[:, 1], twist_cos, twist_sin
        )
        evolve_rows = lax.all_to_all(
            jnp.stack((forward_real_part, forward_imag_part), axis=1),
            "freq",
            split_axis=4,
            concat_axis=4,
            tiled=True,
        )
        flat = evolve_rows.reshape(evolve_rows.shape[0], 2, mode_count, local_count)
        spectrum = transform(flat, long_cos, long_sin)
        spec_real = spectrum[:, 0]
        spec_imag = spectrum[:, 1]
        mixed_real = jnp.einsum(
            "nmk,bmk->bnk", mixing_real, spec_real, precision=HIGHEST
        ) - jnp.einsum("nmk,bmk->bnk", mixing_imag, spec_imag, precision=HIGHEST)
        mixed_imag = jnp.einsum(
            "nmk,bmk->bnk", mixing_real, spec_imag, precision=HIGHEST
        ) + jnp.einsum("nmk,bmk->bnk", mixing_imag, spec_real, precision=HIGHEST)
        real_part, imag_part = rotate(mixed_real, mixed_imag, spread_cos, spread_sin)
        inverted = transform(
            jnp.stack((real_part, imag_part), axis=1), inverse_long_cos, inverse_long_sin
        )
        real_part, imag_part = rotate(inverted[:, 0], inverted[:, 1], untwist_cos, untwist_sin)
        moved = jnp.stack((real_part, imag_part), axis=1).reshape(evolve_rows.shape)
        columns = nonlinear_phase(
            transform(
                lax.all_to_all(moved, "freq", split_axis=4, concat_axis=4, tiled=True),
                inverse_short_cos,
                inverse_short_sin,
            )
            * (1.0 / total_count),
            kerr_gain,
        )
    returned = lax.all_to_all(columns, "freq", split_axis=4, concat_axis=4, tiled=True)
    return returned.reshape(columns.shape[0], 2, mode_count, local_count)


LANES = 128
HALF = LANES // 2
SUB = 8
ROW = 16
GROUPS = ((0, 1), (1, 3), (3, 4))


def low_lanes(shape):
    return lax.broadcasted_iota(jnp.int32, shape, len(shape) - 1) < HALF


def swap(x):
    return pltpu.roll(x, HALF, x.ndim - 1)


def sign_row(rows):
    return jnp.where(low_lanes((rows, LANES)), -1.0, 1.0).astype(jnp.float32)


def times_root(x, index, count, orient, sgn):
    eighth = 8 * index
    if index == 0:
        return x
    if eighth == 2 * count:
        return swap(x) * (sgn * orient)
    angle = 2.0 * np.pi * index / count
    return x * float(np.cos(angle)) + swap(x) * (sgn * float(orient * np.sin(angle)))


def short_fft(items, orient, sgn):
    count = len(items)
    if count == 1:
        return items
    even = short_fft(items[0::2], orient, sgn)
    odd = short_fft(items[1::2], orient, sgn)
    turned = [times_root(v, k, count, orient, sgn) for k, v in enumerate(odd)]
    return [e + t for e, t in zip(even, turned)] + [e - t for e, t in zip(even, turned)]


def packed_mul(x, cosine, signed_sine):
    return x * cosine + swap(x) * signed_sine


def split_constant(value, pieces, bits):
    parts = []
    for _ in range(pieces - 1):
        exponent = np.floor(np.log2(value))
        unit = 2.0 ** (exponent - bits + 1)
        part = np.floor(value / unit) * unit
        parts.append(float(part))
        value -= part
    return parts + [float(value)]


HALF_PI = split_constant(np.pi / 2, 4, 8)


def sine_cosine(theta):
    turns = jnp.floor(theta * float(2 / np.pi) + 0.5)
    rest = theta
    for part in HALF_PI:
        rest = rest - turns * part
    square = rest * rest
    sine = rest + rest * square * (
        -1.6666654611e-1 + square * (8.3321608736e-3 - square * 1.9515295891e-4)
    )
    cosine = 1.0 - 0.5 * square + square * square * (
        4.166664568298827e-2 + square * (-1.388731625493765e-3 + square * 2.443315711809948e-5)
    )
    quadrant = turns.astype(jnp.int32) & 3
    crossed = (quadrant & 1) == 1
    out_sine = jnp.where(crossed, cosine, sine)
    out_cosine = jnp.where(crossed, sine, cosine)
    out_sine = jnp.where(quadrant >= 2, -out_sine, out_sine)
    out_cosine = jnp.where((quadrant == 1) | (quadrant == 2), -out_cosine, out_cosine)
    return out_sine, out_cosine


def long_dft(x, weights):
    high = x.astype(jnp.bfloat16)
    low = (x - high.astype(jnp.float32)).astype(jnp.bfloat16)
    both = jnp.concatenate((high, low), axis=1)
    product = jnp.dot(both, weights, preferred_element_type=jnp.float32)
    return product[:, :LANES] + product[:, LANES:]


def trade(vectors, stride, shift):
    lane = lax.broadcasted_iota(jnp.int32, (SUB, LANES), 1)
    lower = (lane // shift) % 2 == 0
    out = list(vectors)
    for k in range(len(vectors)):
        if (k // stride) % 2 == 0:
            first, second = vectors[k], vectors[k + stride]
            out[k] = jnp.where(lower, first, pltpu.roll(second, shift, 1))
            out[k + stride] = jnp.where(lower, pltpu.roll(first, LANES - shift, 1), second)
    return out


def mega_kernel(
    count, modes, scale, groups, pulse_ref, c_hbm, terms_ref, gain_in, tw_cos_ref, tw_sin_ref,
    fwd_ref, inv_ref, out_ref, c_ref, early, recv, late, send, spec, by_real, by_imag, total, field,
    acc, spread_cos_ref, spread_sin_ref, twist_cos_ref, twist_sin_ref, gain_ref,
    send_sem, recv_sem, c_sem,
):
    me = lax.axis_index("freq")
    chunks = recv.shape[2] // SUB
    rows = recv.shape[2]
    width = c_ref.shape[2]
    pitch = by_real.shape[0] // rows
    span = early.shape[0] // count
    sgn = sign_row(SUB)
    low = low_lanes((SUB, LANES))
    odd = lax.broadcasted_iota(jnp.int32, (SUB, LANES), 0) % 2 == 1
    exchanges = recv.shape[0] + 1

    def tile_rows(c):
        return pl.ds(pl.multiple_of(c * SUB, SUB), SUB)

    def block_of(ref):
        return lambda peer, row, size: ref.at[peer, pl.ds(row, size)]

    def flat_of(ref):
        return lambda peer, row, size: ref.at[pl.ds(pl.multiple_of(peer * span + row, SUB), size)]

    def landing(ex):
        return flat_of(late) if ex == exchanges - 1 else block_of(recv.at[ex])

    def remote(src, dst, ex, g, peer):
        return pltpu.make_async_remote_copy(
            src_ref=src,
            dst_ref=dst,
            send_sem=send_sem.at[ex],
            recv_sem=recv_sem.at[ex, g],
            device_id=(peer,),
            device_id_type=pl.DeviceIdType.MESH,
        )

    def extent(g):
        start, end = groups[g]
        return start * SUB, min(end * SUB, modes) - start * SUB

    def post(src, ex, c):
        dst = landing(ex)
        for g, (_, end) in enumerate(groups):
            row, size = extent(g)

            def go(row=row, size=size, g=g):
                dst(me, row, size)[...] = src(me, row, size)[...]

                def one(j, carry):
                    k = count - j
                    peer = 0
                    for b in range(count.bit_length() - 1):
                        mine = (me // (1 << b)) % 2
                        peer = peer + ((k // (1 << b) + mine) % 2) * (1 << b)
                    remote(src(peer, row, size), dst(me, row, size), ex, g, peer).start()
                    return carry

                lax.fori_loop(1, count, one, 0)

            pl.when(c == end - 1)(go)

    def arrive(ex, c):
        for g, (start, _) in enumerate(groups):
            row, size = extent(g)

            def go(row=row, size=size, g=g):
                if ex == exchanges - 1:
                    part = late.at[pl.ds(0, (count - 1) * size)]
                else:
                    part = recv.at[ex, pl.ds(0, count - 1), pl.ds(row, size)]
                remote(part, part, ex, g, (me + 1) % count).wait_recv()

            pl.when(c == start)(go)

    def each(body):
        def step(c, carry):
            body(c)
            return carry

        lax.fori_loop(0, chunks, step, 0)

    load = pltpu.make_async_copy(c_hbm, c_ref, c_sem)
    load.start()
    barrier = pltpu.get_barrier_semaphore()

    def greet(k, carry):
        pl.semaphore_signal(
            barrier, inc=1, device_id=((me + k) % count,), device_id_type=pl.DeviceIdType.MESH
        )
        return carry

    lax.fori_loop(1, count, greet, 0)
    if rows > modes:
        spare = pl.ds(modes, rows - modes)
        for ex in range(exchanges - 1):
            recv[ex, :, spare, :] = jnp.zeros((count, rows - modes, LANES), jnp.float32)
    total[...] = jnp.zeros_like(total)

    def unpack(q):
        names = [min(4 * q + i, modes - 1) for i in range(4)]
        pieces = [
            pulse_ref[m, pl.ds(ri + 2 * SUB * half, SUB, stride=2), :]
            for ri in range(2)
            for m in names
            for half in range(2)
        ]
        turned = jnp.concatenate(pieces, axis=0).T
        for eb in range(count // SUB):
            parts = [turned[gl * count + eb * SUB : gl * count + eb * SUB + SUB] for gl in range(4)]
            parts = trade(trade(parts, 2, 2 * ROW), 1, ROW)
            for i in range(4):
                if 4 * q + i < modes:
                    early[pl.ds(eb * SUB * span + 4 * q + i, SUB, stride=span), :] = parts[i]

    def repack(q):
        names = [min(4 * q + i, modes - 1) for i in range(4)]
        pieces = [[] for _ in range(4)]
        for eb in range(count // SUB):
            parts = [late[pl.ds(eb * SUB * span + m, SUB, stride=span), :] for m in names]
            parts = trade(trade(parts, 1, ROW), 2, 2 * ROW)
            for gl in range(4):
                pieces[gl].append(parts[gl])
        turned = jnp.concatenate([p for piece in pieces for p in piece], axis=0).T
        for ri in range(2):
            for i in range(4):
                if 4 * q + i < modes:
                    for half in range(2):
                        at = (ri * 4 + i) * ROW + half * SUB
                        out_ref[4 * q + i, pl.ds(ri + 2 * SUB * half, SUB, stride=2), :] = turned[
                            at : at + SUB
                        ]

    for q in range(2 * groups[0][1]):
        unpack(q)
    pl.semaphore_wait(barrier, count - 1)
    for c in range(chunks):
        if c >= groups[0][1]:
            unpack(2 * c)
            unpack(2 * c + 1)
        if c in [end - 1 for _, end in groups]:
            post(flat_of(early), 0, c)

    lane = lax.broadcasted_iota(jnp.int32, (SUB, LANES), 1)
    line = lax.broadcasted_iota(jnp.int32, (SUB, LANES), 0)
    place = lane % HALF
    sample = me + count * (place % ROW * 4 + place // ROW)
    total_count = count * count * HALF
    for c in range(count // SUB):
        turns = (line + c * SUB) * sample
        sine, cosine = sine_cosine(turns.astype(jnp.float32) * (2.0 * np.pi / total_count))
        twist_cos_ref[tile_rows(c), :] = cosine
        twist_sin_ref[tile_rows(c), :] = sine * -sgn

    def by_mode(read, c):
        value = jnp.zeros((SUB, LANES), jnp.float32)
        for r in range(min(SUB, modes - c * SUB)):
            value = jnp.where(line == r, read(c * SUB + r), value)
        return value

    for c in range(chunks):
        gain_ref[tile_rows(c), :] = by_mode(lambda m: gain_in[m], c)
        factors = [by_mode(lambda m: terms_ref[k, m], c) for k in range(3)]

        def spread(tile, carry):
            bins = me + count * (tile * LANES + lane)
            signed = jnp.where(bins < total_count // 2, bins, bins - total_count)
            angular = signed.astype(jnp.float32) * (2.0 / total_count)
            square = angular * angular
            phase = (
                factors[0] * angular + factors[1] * square / 2 + factors[2] * (square * angular) / 6
            )
            sine, cosine = sine_cosine(phase)
            lanes = pl.ds(pl.multiple_of(tile * LANES, LANES), LANES)
            spread_cos_ref[tile_rows(c), lanes] = cosine
            spread_sin_ref[tile_rows(c), lanes] = sine
            return carry

        lax.fori_loop(0, width // 2, spread, 0, unroll=4)

    def columns_out(source, dst, ex, c):
        at = tile_rows(c)
        items = short_fft([source[a, at, :] for a in range(count)], -1.0, sgn)
        for d, value in enumerate(items):
            dst[d, at, :] = packed_mul(value, twist_cos_ref[d : d + 1, :], twist_sin_ref[d : d + 1, :])
        post(block_of(dst), ex, c)

    def row_in(ex, c):
        at = tile_rows(c)
        block = recv[ex, :, at, :].reshape(count * SUB, LANES)
        spec[...] = long_dft(block, fwd_ref[...]).reshape(count, SUB, LANES)
        items = short_fft(
            [
                packed_mul(spec[p], tw_cos_ref[p : p + 1, :], tw_sin_ref[p : p + 1, :])
                for p in range(count)
            ],
            -1.0,
            sgn,
        )
        for tile in range(width // 2):
            first, second = items[2 * tile], items[2 * tile + 1]
            real = jnp.where(low, first, swap(second))
            imag = jnp.where(low, swap(first), second)
            for part in range(2):
                to = pl.ds(c * SUB * pitch + 2 * tile + part, SUB, stride=pitch)
                by_real[to, :] = real
                by_imag[to, :] = imag

    def mix(c, size):
        def body(q, carry):
            def spot(index):
                return pl.ds(pl.multiple_of(index * pitch + q * SUB, SUB), SUB)

            with_real = [
                jnp.where(odd, by_imag[spot(c * SUB + g), :], by_real[spot(c * SUB + g), :])
                for g in range(size)
            ]
            with_imag = [jnp.zeros((SUB, LANES), jnp.float32) for _ in range(size)]
            for m in range(modes):
                real, imag = by_real[spot(m), :], by_imag[spot(m), :]
                for g in range(size):
                    factor = c_ref[c * SUB + g, m, tile_rows(q), :]
                    with_real[g] = with_real[g] + factor * real
                    with_imag[g] = with_imag[g] + factor * imag
            for g in range(size):
                other = jnp.where(
                    odd, pltpu.roll(with_imag[g], 1, 0), -pltpu.roll(with_imag[g], SUB - 1, 0)
                )
                total[spot(g), :] = with_real[g] + other
            return carry

        lax.fori_loop(0, width // SUB, body, 0)

    def row_out(dst, ex, c):
        at = tile_rows(c)
        if modes % SUB == 0:
            mix(c, SUB)
        else:
            pl.when(c < chunks - 1)(lambda: mix(c, SUB))
            pl.when(c == chunks - 1)(lambda: mix(c, modes % SUB))
        items = []
        for tile in range(width // 2):
            lanes = pl.ds(tile * LANES, LANES)
            real, imag = rotate(
                total[pl.ds(2 * tile, SUB, stride=pitch), :],
                total[pl.ds(2 * tile + 1, SUB, stride=pitch), :],
                spread_cos_ref[at, lanes],
                spread_sin_ref[at, lanes],
            )
            items.append(jnp.where(low, real, swap(imag)))
            items.append(jnp.where(low, swap(real), imag))
        for p, value in enumerate(short_fft(items, 1.0, sgn)):
            spec[p] = packed_mul(value, tw_cos_ref[p : p + 1, :], -tw_sin_ref[p : p + 1, :])
        block = spec[...].reshape(count * SUB, LANES)
        dst[:, at, :] = long_dft(block, inv_ref[...]).reshape(count, SUB, LANES)
        post(block_of(dst), ex, c)

    def columns_in(ex, c):
        at = tile_rows(c)
        items = [
            packed_mul(
                recv[ex, d, at, :],
                twist_cos_ref[d : d + 1, :],
                -twist_sin_ref[d : d + 1, :],
            )
            for d in range(count)
        ]
        for a, value in enumerate(short_fft(items, 1.0, sgn)):
            field[a, at, :] = value
            acc[a] = acc[a] + value * value

    def power():
        def body(k, carry):
            at = pl.ds(k * SUB, SUB)
            part = jnp.sum(acc[at], axis=1, keepdims=True)
            acc[at] = jnp.broadcast_to(2.0 * (part + swap(part)), (SUB, SUB, LANES))
            return carry

        lax.fori_loop(0, count // SUB, body, 0)

    def kerr(target, c):
        at = tile_rows(c)
        gain = gain_ref[at, :]

        def body(k, carry):
            first, second = pl.ds(k * SUB, SUB // 2), pl.ds(k * SUB + SUB // 2, SUB // 2)
            values, angles = [], []
            for part in (first, second):
                x = field[part, at, :]
                square = x * x
                values.append(x)
                angles.append(acc[part] - (square + swap(square)))
            sine, cosine = sine_cosine(gain * jnp.where(low, angles[0], angles[1]))
            other_sine, other_cosine = swap(sine), swap(cosine)
            pairs = (
                (jnp.where(low, cosine, other_cosine), jnp.where(low, -sine, other_sine)),
                (jnp.where(low, other_cosine, cosine), jnp.where(low, -other_sine, sine)),
            )
            for part, x, (cosines, sines) in zip((first, second), values, pairs):
                target[part, at, :] = packed_mul(x, cosines, sines)
            return carry

        lax.fori_loop(0, count // SUB, body, 0)

    ex = 1
    for repeat in range(STEPS):
        dst = send.at[ex - 1]
        if repeat == 0:

            def begin(c):
                arrive(0, c)
                columns_out(recv.at[0], dst, ex, c)

            each(begin)
        else:
            power()

            def bend(c):
                kerr(field, c)
                columns_out(field, dst, ex, c)

            each(bend)

        def inward(c):
            arrive(ex, c)
            row_in(ex, c)

        each(inward)
        if repeat == 0:
            load.wait()
        ex += 1
        each(lambda c: row_out(send.at[ex - 1], ex, c))
        acc[...] = jnp.zeros_like(acc)

        def collect(c):
            arrive(ex, c)
            columns_in(ex, c)

        each(collect)
        ex += 1
    power()

    def finish(c):
        kerr(send.at[ex - 1], c)
        post(block_of(send.at[ex - 1]), ex, c)

    each(finish)

    for c in range(chunks):
        arrive(ex, c)
        repack(2 * c)
        if 4 * (2 * c + 1) < modes:
            repack(2 * c + 1)
    for ex in range(exchanges):
        sent = send.at[0, pl.ds(0, count - 1), pl.ds(0, modes)]
        remote(sent, sent, ex, 0, (me + 1) % count).wait_send()


def mega(pulses, coupling, terms, gain, tw_cos, tw_sin, fwd, inv, count, scale):
    modes, width = coupling.shape[0], coupling.shape[2]
    rows = -(-modes // SUB) * SUB
    pitch = width + SUB
    exchanges = 2 * STEPS + 2
    vmem = pl.BlockSpec(memory_space=pltpu.VMEM)
    smem = pl.BlockSpec(memory_space=pltpu.SMEM)
    block = (count, rows, LANES)
    tiles = rows // SUB
    groups = GROUPS if tiles == 4 else ((0, tiles),)
    flat = (count * (rows + SUB), LANES)
    mixed = (rows * pitch, LANES)
    return pl.pallas_call(
        functools.partial(mega_kernel, count, modes, scale, groups),
        out_shape=jax.ShapeDtypeStruct(pulses.shape, pulses.dtype),
        in_specs=[vmem, pl.BlockSpec(memory_space=pl.ANY), smem, smem] + [vmem] * 4,
        out_specs=vmem,
        scratch_shapes=[
            pltpu.VMEM(coupling.shape, jnp.float32),
            pltpu.VMEM(flat, jnp.float32),
            pltpu.VMEM((exchanges - 1,) + block, jnp.float32),
            pltpu.VMEM(flat, jnp.float32),
            pltpu.VMEM((exchanges - 1,) + block, jnp.float32),
            pltpu.VMEM((count, SUB, LANES), jnp.float32),
            pltpu.VMEM(mixed, jnp.float32),
            pltpu.VMEM(mixed, jnp.float32),
            pltpu.VMEM((SUB * pitch, LANES), jnp.float32),
            pltpu.VMEM(block, jnp.float32),
            pltpu.VMEM((count, SUB, LANES), jnp.float32),
            pltpu.VMEM((rows, width // 2 * LANES), jnp.float32),
            pltpu.VMEM((rows, width // 2 * LANES), jnp.float32),
            pltpu.VMEM((count, LANES), jnp.float32),
            pltpu.VMEM((count, LANES), jnp.float32),
            pltpu.VMEM((rows, LANES), jnp.float32),
            pltpu.SemaphoreType.DMA((exchanges,)),
            pltpu.SemaphoreType.DMA((exchanges, len(groups))),
            pltpu.SemaphoreType.DMA(()),
        ],
        compiler_params=pltpu.CompilerParams(collective_id=0, has_side_effects=True),
        name="mega",
    )(pulses, coupling, terms, gain, tw_cos, tw_sin, fwd, inv)


def packed_table(cosine, sine):
    xp = np if isinstance(cosine, np.ndarray) else jnp
    return (
        xp.concatenate((cosine, cosine), axis=1).astype(xp.float32),
        xp.concatenate((-sine, sine), axis=1).astype(xp.float32),
    )


def lane_order(size):
    place = np.arange(size)
    return place % ROW * (size // ROW) + place // ROW


def dft_weights(size, orient, scale):
    first, second = lane_order(size), np.arange(size)
    if orient > 0:
        first, second = second, first
    angle = orient * 2.0 * np.pi * (first[:, None] * second[None, :] % size) / size
    cosine, sine = scale * np.cos(angle), scale * np.sin(angle)
    full = np.block([[cosine, sine], [-sine, cosine]]).astype(np.float32)
    high = full.astype(jnp.bfloat16)
    low = (full - high.astype(np.float32)).astype(jnp.bfloat16)
    return np.block([[high, low], [high, np.zeros_like(low)]])


def packed_device(pulses, coupling, dispersion_terms, kerr_gain):
    shards = lax.axis_size("freq")
    modes, local = pulses.shape[2], pulses.shape[3]
    groups = local // shards
    tiles = local // LANES
    scale = 1.0 / (local * shards)

    shard_index = np.arange(shards)
    angle = -2.0 * np.pi * (shard_index[:, None] * np.arange(groups)[None, :] % local) / local
    tw_cos, tw_sin = packed_table(np.cos(angle), np.sin(angle))
    fwd, inv = dft_weights(groups, -1.0, 1.0), dft_weights(groups, 1.0, scale)
    coupling = coupling.reshape(2, modes, modes, tiles, LANES).transpose(1, 2, 3, 0, 4)
    coupling = coupling.reshape(modes, modes, 2 * tiles, LANES)
    x = pulses.reshape(2, modes, tiles, LANES).transpose(1, 2, 0, 3).reshape(modes, 2 * tiles, LANES)
    x = mega(x, coupling, dispersion_terms, kerr_gain, tw_cos, tw_sin, fwd, inv, shards, scale)
    x = x.reshape(modes, tiles, 2, LANES).transpose(2, 0, 1, 3)
    return x.reshape(1, 2, modes, local)


def fits(shards, pulses):
    local = pulses.shape[3] // shards
    return (
        pulses.shape[0] == 1
        and shards & (shards - 1) == 0
        and shards == 2 * ROW
        and local == shards * HALF
    )


def solution(mesh):
    in_specs = (P(None, None, None, "freq"), P(None, None, None, "freq"), P(), P())
    out_specs = P(None, None, None, "freq")
    shards = mesh.shape["freq"]

    def run(pulses, coupling, dispersion_terms, kerr_gain):
        body = packed_device if fits(shards, pulses) else per_device
        return jax.shard_map(
            body, mesh=mesh, in_specs=in_specs, out_specs=out_specs, check_vma=False
        )(pulses, coupling, dispersion_terms, kerr_gain)

    return run
```

```python
import functools

import jax
import jax.numpy as jnp
import numpy as np
from jax import lax
from jax.experimental import pallas as pl
from jax.experimental.pallas import tpu as pltpu
from jax.sharding import PartitionSpec as P

STEPS = 2


HIGHEST = lax.Precision.HIGHEST


def angle_table(first, second, modulus, orient):
    turns = first[:, None] * second[None, :] % modulus
    radians = turns.astype(jnp.float32) * (2.0 * jnp.pi / modulus)
    return (jnp.cos(radians), orient * jnp.sin(radians))


def rotate(real_part, imag_part, cosine, sine):
    return (real_part * cosine - imag_part * sine, real_part * sine + imag_part * cosine)


def transform(stacked, cosine, sine):
    real_part = stacked[:, 0]
    imag_part = stacked[:, 1]
    out_real = jnp.matmul(real_part, cosine, precision=HIGHEST) - jnp.matmul(
        imag_part, sine, precision=HIGHEST
    )
    out_imag = jnp.matmul(real_part, sine, precision=HIGHEST) + jnp.matmul(
        imag_part, cosine, precision=HIGHEST
    )
    return jnp.stack((out_real, out_imag), axis=1)


def nonlinear_phase(stacked, kerr_gain):
    magnitude = stacked[:, 0] ** 2 + stacked[:, 1] ** 2
    total_power = jnp.sum(magnitude, axis=1, keepdims=True)
    gains = kerr_gain.reshape((1, -1) + (1,) * (magnitude.ndim - 2))
    angles = gains * (2.0 * total_power - magnitude)
    real_part, imag_part = rotate(stacked[:, 0], stacked[:, 1], jnp.cos(angles), jnp.sin(angles))
    return jnp.stack((real_part, imag_part), axis=1)


def per_device(pulses, coupling, dispersion_terms, kerr_gain):
    shards = lax.axis_size("freq")
    device = lax.axis_index("freq")
    mode_count = pulses.shape[2]
    local_count = pulses.shape[3]
    groups = local_count // shards
    total_count = local_count * shards
    column_index = jnp.arange(shards, dtype=jnp.int32)
    row_index = jnp.arange(local_count, dtype=jnp.int32)
    short_cos, short_sin = angle_table(column_index, column_index, shards, -1.0)
    inverse_short_cos, inverse_short_sin = angle_table(column_index, column_index, shards, 1.0)
    long_cos, long_sin = angle_table(row_index, row_index, local_count, -1.0)
    inverse_long_cos, inverse_long_sin = angle_table(row_index, row_index, local_count, 1.0)
    sample_rows = jnp.arange(groups, dtype=jnp.int32) * shards + device
    twist_cos, twist_sin = angle_table(sample_rows, column_index, total_count, -1.0)
    untwist_cos, untwist_sin = angle_table(row_index, jnp.reshape(device, (1,)), total_count, 1.0)
    untwist_cos = untwist_cos.reshape(-1)
    untwist_sin = untwist_sin.reshape(-1)
    bins = device + shards * row_index
    signed_bin = jnp.where(bins < total_count // 2, bins, bins - total_count).astype(jnp.float32)
    angular = signed_bin / (total_count // 2)
    dispersion = (
        dispersion_terms[0][:, None] * angular
        + dispersion_terms[1][:, None] * angular**2 / 2
        + dispersion_terms[2][:, None] * angular**3 / 6
    )
    spread_cos = jnp.cos(dispersion)
    spread_sin = jnp.sin(dispersion)
    identity = jnp.eye(mode_count, dtype=jnp.float32)[:, :, None]
    mixing_real = coupling[0] + identity
    mixing_imag = coupling[1]
    blocks = pulses.reshape(pulses.shape[0], 2, mode_count, groups, shards)
    columns = lax.all_to_all(blocks, "freq", split_axis=4, concat_axis=4, tiled=True)
    for repeat in range(STEPS):
        spectral = transform(columns, short_cos, short_sin)
        forward_real_part, forward_imag_part = rotate(
            spectral[:, 0], spectral[:, 1], twist_cos, twist_sin
        )
        evolve_rows = lax.all_to_all(
            jnp.stack((forward_real_part, forward_imag_part), axis=1),
            "freq",
            split_axis=4,
            concat_axis=4,
            tiled=True,
        )
        flat = evolve_rows.reshape(evolve_rows.shape[0], 2, mode_count, local_count)
        spectrum = transform(flat, long_cos, long_sin)
        spec_real = spectrum[:, 0]
        spec_imag = spectrum[:, 1]
        mixed_real = jnp.einsum(
            "nmk,bmk->bnk", mixing_real, spec_real, precision=HIGHEST
        ) - jnp.einsum("nmk,bmk->bnk", mixing_imag, spec_imag, precision=HIGHEST)
        mixed_imag = jnp.einsum(
            "nmk,bmk->bnk", mixing_real, spec_imag, precision=HIGHEST
        ) + jnp.einsum("nmk,bmk->bnk", mixing_imag, spec_real, precision=HIGHEST)
        real_part, imag_part = rotate(mixed_real, mixed_imag, spread_cos, spread_sin)
        inverted = transform(
            jnp.stack((real_part, imag_part), axis=1), inverse_long_cos, inverse_long_sin
        )
        real_part, imag_part = rotate(inverted[:, 0], inverted[:, 1], untwist_cos, untwist_sin)
        moved = jnp.stack((real_part, imag_part), axis=1).reshape(evolve_rows.shape)
        columns = nonlinear_phase(
            transform(
                lax.all_to_all(moved, "freq", split_axis=4, concat_axis=4, tiled=True),
                inverse_short_cos,
                inverse_short_sin,
            )
            * (1.0 / total_count),
            kerr_gain,
        )
    returned = lax.all_to_all(columns, "freq", split_axis=4, concat_axis=4, tiled=True)
    return returned.reshape(columns.shape[0], 2, mode_count, local_count)


LANES = 128
HALF = LANES // 2
SUB = 8
ROW = 16
CLASSES = 2
GROUPS = (((0, 1), (1, 2), (2, 3), (3, 4)),) * 6


def low_lanes(shape):
    return lax.broadcasted_iota(jnp.int32, shape, len(shape) - 1) < HALF


def swap(x):
    return pltpu.roll(x, HALF, x.ndim - 1)


def sign_row(rows):
    return jnp.where(low_lanes((rows, LANES)), -1.0, 1.0).astype(jnp.float32)


def times_root(x, index, count, orient, sgn):
    eighth = 8 * index
    if index == 0:
        return x
    if eighth == 2 * count:
        return swap(x) * (sgn * orient)
    angle = 2.0 * np.pi * index / count
    return x * float(np.cos(angle)) + swap(x) * (sgn * float(orient * np.sin(angle)))


def short_fft(items, orient, sgn):
    count = len(items)
    if count == 1:
        return items
    even = short_fft(items[0::2], orient, sgn)
    odd = short_fft(items[1::2], orient, sgn)
    turned = [times_root(v, k, count, orient, sgn) for k, v in enumerate(odd)]
    return [e + t for e, t in zip(even, turned)] + [e - t for e, t in zip(even, turned)]


def packed_mul(x, cosine, signed_sine):
    return x * cosine + swap(x) * signed_sine


def split_constant(value, pieces, bits):
    parts = []
    for _ in range(pieces - 1):
        exponent = np.floor(np.log2(value))
        unit = 2.0 ** (exponent - bits + 1)
        part = np.floor(value / unit) * unit
        parts.append(float(part))
        value -= part
    return parts + [float(value)]


HALF_PI = split_constant(np.pi / 2, 4, 8)


def sine_cosine(theta):
    turns = jnp.floor(theta * float(2 / np.pi) + 0.5)
    rest = theta
    for part in HALF_PI:
        rest = rest - turns * part
    square = rest * rest
    sine = rest + rest * square * (
        -1.6666654611e-1 + square * (8.3321608736e-3 - square * 1.9515295891e-4)
    )
    cosine = 1.0 - 0.5 * square + square * square * (
        4.166664568298827e-2 + square * (-1.388731625493765e-3 + square * 2.443315711809948e-5)
    )
    quadrant = turns.astype(jnp.int32) & 3
    crossed = (quadrant & 1) == 1
    out_sine = jnp.where(crossed, cosine, sine)
    out_cosine = jnp.where(crossed, sine, cosine)
    out_sine = jnp.where(quadrant >= 2, -out_sine, out_sine)
    out_cosine = jnp.where((quadrant == 1) | (quadrant == 2), -out_cosine, out_cosine)
    return out_sine, out_cosine


def long_dft(x, weights):
    high = x.astype(jnp.bfloat16)
    low = (x - high.astype(jnp.float32)).astype(jnp.bfloat16)
    both = jnp.concatenate((high, low), axis=1)
    product = jnp.dot(both, weights, preferred_element_type=jnp.float32)
    return product[:, :LANES] + product[:, LANES:]


def trade(vectors, stride, shift):
    lane = lax.broadcasted_iota(jnp.int32, (SUB, LANES), 1)
    lower = (lane // shift) % 2 == 0
    out = list(vectors)
    for k in range(len(vectors)):
        if (k // stride) % 2 == 0:
            first, second = vectors[k], vectors[k + stride]
            out[k] = jnp.where(lower, first, pltpu.roll(second, shift, 1))
            out[k + stride] = jnp.where(lower, pltpu.roll(first, LANES - shift, 1), second)
    return out


def mega_kernel(
    count, modes, scale, groups, pulse_hbm, c_hbm, terms_ref, gain_in, tw_cos_ref, tw_sin_ref,
    fwd_ref, inv_ref, out_ref, pulse_ref, c_ref, early, recv, late, send, spec, by_real, by_imag, total, field,
    acc, spread_cos_ref, spread_sin_ref, twist_cos_ref, twist_sin_ref, gain_ref,
    send_sem, recv_sem, c_sem,
):
    me = lax.axis_index("freq")
    barrier = pltpu.get_barrier_semaphore()

    def greet(k, carry):
        pl.semaphore_signal(
            barrier, inc=1, device_id=((me + k) % count,), device_id_type=pl.DeviceIdType.MESH
        )
        return carry

    lax.fori_loop(1, count, greet, 0)
    fetch = pltpu.make_async_copy(pulse_hbm, pulse_ref, c_sem.at[0])
    fetch.start()
    load = pltpu.make_async_copy(c_hbm, c_ref, c_sem.at[1])
    load.start()
    chunks = recv.shape[2] // SUB
    rows = recv.shape[2]
    width = c_ref.shape[2]
    pitch = by_real.shape[0] // rows
    span = early.shape[0] // count
    sgn = sign_row(SUB)
    low = low_lanes((SUB, LANES))
    odd = lax.broadcasted_iota(jnp.int32, (SUB, LANES), 0) % 2 == 1
    exchanges = recv.shape[0] + 1

    near = 8
    outer_peers = []
    for k in reversed(range(count // near)):
        place = 0
        for b in range((count // near).bit_length() - 1):
            place = place + ((me // (near << b) + (k >> b)) % 2) * (near << b)
        outer_peers.append(place)
    own_low = me % CLASSES
    step_bits = [(me // (CLASSES << b)) % 2 for b in range((near // CLASSES).bit_length() - 1)]

    def inner_peer(j):
        place = 0
        for b, mine in enumerate(step_bits):
            place = place + ((j // (1 << b) + mine) % 2) * (CLASSES << b)
        return place

    def tile_rows(c):
        return pl.ds(pl.multiple_of(c * SUB, SUB), SUB)

    def block_of(ref):
        return lambda peer, row, size: ref.at[peer, pl.ds(row, size)]

    def flat_of(ref):
        return lambda peer, row, size: ref.at[pl.ds(pl.multiple_of(peer * span + row, SUB), size)]

    def landing(ex):
        return flat_of(late) if ex == exchanges - 1 else block_of(recv.at[ex])

    def remote(src, dst, ex, g, peer):
        return pltpu.make_async_remote_copy(
            src_ref=src,
            dst_ref=dst,
            send_sem=send_sem.at[ex],
            recv_sem=recv_sem.at[ex, g],
            device_id=(peer,),
            device_id_type=pl.DeviceIdType.MESH,
        )

    def extent(ex, g):
        start, end = groups[ex][g]
        return start * SUB, min(end * SUB, modes) - start * SUB

    def post(src, ex, c, kind):
        dst = landing(ex)
        for g, (_, end) in enumerate(groups[ex]):
            row, size = extent(ex, g)

            def go(row=row, size=size, g=g):
                def one(peer):
                    remote(src(peer, row, size), dst(me, row, size), ex, g, peer).start()

                def several(j, carry):
                    inner = inner_peer(near // CLASSES - j)
                    for outer in outer_peers:
                        one(outer + inner + kind)
                    return carry

                lax.fori_loop(1, near // CLASSES, several, 0)
                inner = inner_peer(0)
                for outer in outer_peers[:-1]:
                    one(outer + inner + kind)
                pl.when(own_low != kind)(lambda: one(outer_peers[-1] + inner + kind))

                @pl.when(own_low == kind)
                def _():
                    dst(me, row, size)[...] = src(me, row, size)[...]

            pl.when(c == end - 1)(go)

    def post_rest(src, ex):
        def body(i, carry):
            post(src, ex, i % chunks, 1 + i // chunks)
            return carry

        lax.fori_loop(0, chunks * (CLASSES - 1), body, 0)

    def arrive(ex, c):
        for g, (start, _) in enumerate(groups[ex]):
            row, size = extent(ex, g)

            def go(row=row, size=size, g=g):
                if ex == exchanges - 1:
                    part = late.at[pl.ds(0, (count - 1) * size)]
                else:
                    part = recv.at[ex, pl.ds(0, count - 1), pl.ds(row, size)]
                remote(part, part, ex, g, (me + 1) % count).wait_recv()

            pl.when(c == start)(go)

    def each(body):
        def step(c, carry):
            body(c)
            return carry

        lax.fori_loop(0, chunks, step, 0)

    if rows > modes:
        spare = pl.ds(modes, rows - modes)
        for ex in range(exchanges - 1):
            recv[ex, :, spare, :] = jnp.zeros((count, rows - modes, LANES), jnp.float32)

    def unpack(q):
        names = [min(4 * q + i, modes - 1) for i in range(4)]
        pieces = [
            pulse_ref[m, pl.ds(ri + 2 * SUB * half, SUB, stride=2), :]
            for ri in range(2)
            for m in names
            for half in range(2)
        ]
        turned = jnp.concatenate(pieces, axis=0).T
        for eb in range(count // SUB):
            parts = [turned[gl * count + eb * SUB : gl * count + eb * SUB + SUB] for gl in range(4)]
            parts = trade(trade(parts, 2, 2 * ROW), 1, ROW)
            for i in range(4):
                if 4 * q + i < modes:
                    early[pl.ds(eb * SUB * span + 4 * q + i, SUB, stride=span), :] = parts[i]

    def repack(q):
        names = [min(4 * q + i, modes - 1) for i in range(4)]
        pieces = [[] for _ in range(4)]
        for eb in range(count // SUB):
            parts = [late[pl.ds(eb * SUB * span + m, SUB, stride=span), :] for m in names]
            parts = trade(trade(parts, 1, ROW), 2, 2 * ROW)
            for gl in range(4):
                pieces[gl].append(parts[gl])
        turned = jnp.concatenate([p for piece in pieces for p in piece], axis=0).T
        for ri in range(2):
            for i in range(4):
                if 4 * q + i < modes:
                    for half in range(2):
                        at = (ri * 4 + i) * ROW + half * SUB
                        out_ref[4 * q + i, pl.ds(ri + 2 * SUB * half, SUB, stride=2), :] = turned[
                            at : at + SUB
                        ]

    fetch.wait()
    for q in range(-(-modes // 4)):
        unpack(q)
    pl.semaphore_wait(barrier, count - 1)
    each(lambda c: post(flat_of(early), 0, c, 0))
    post_rest(flat_of(early), 0)

    lane = lax.broadcasted_iota(jnp.int32, (SUB, LANES), 1)
    line = lax.broadcasted_iota(jnp.int32, (SUB, LANES), 0)
    place = lane % HALF
    sample = me + count * (place % ROW * 4 + place // ROW)
    total_count = count * count * HALF
    for c in range(count // SUB):
        turns = (line + c * SUB) * sample
        sine, cosine = sine_cosine(turns.astype(jnp.float32) * (2.0 * np.pi / total_count))
        twist_cos_ref[tile_rows(c), :] = cosine
        twist_sin_ref[tile_rows(c), :] = sine * -sgn

    def by_mode(read, c):
        value = jnp.zeros((SUB, LANES), jnp.float32)
        for r in range(min(SUB, modes - c * SUB)):
            value = jnp.where(line == r, read(c * SUB + r), value)
        return value

    for c in range(chunks):
        gain_ref[tile_rows(c), :] = by_mode(lambda m: gain_in[m], c)
        factors = [by_mode(lambda m: terms_ref[k, m], c) for k in range(3)]

        def spread(tile, carry):
            bins = me + count * (tile * LANES + lane)
            signed = jnp.where(bins < total_count // 2, bins, bins - total_count)
            angular = signed.astype(jnp.float32) * (2.0 / total_count)
            square = angular * angular
            phase = (
                factors[0] * angular + factors[1] * square / 2 + factors[2] * (square * angular) / 6
            )
            sine, cosine = sine_cosine(phase)
            lanes = pl.ds(pl.multiple_of(tile * LANES, LANES), LANES)
            spread_cos_ref[tile_rows(c), lanes] = cosine
            spread_sin_ref[tile_rows(c), lanes] = sine
            return carry

        lax.fori_loop(0, width // 2, spread, 0, unroll=4)
    total[...] = jnp.zeros_like(total)

    def columns_out(source, where, dst, ex, c):
        at = tile_rows(c)
        items = short_fft([source[a, where, :] for a in range(count)], -1.0, sgn)
        for d, value in enumerate(items):
            dst[d, at, :] = packed_mul(value, twist_cos_ref[d : d + 1, :], twist_sin_ref[d : d + 1, :])
        post(block_of(dst), ex, c, 0)

    def row_in(ex, c):
        at = tile_rows(c)
        block = recv[ex, :, at, :].reshape(count * SUB, LANES)
        spec[...] = long_dft(block, fwd_ref[...]).reshape(count, SUB, LANES)
        items = short_fft(
            [
                packed_mul(spec[p], tw_cos_ref[p : p + 1, :], tw_sin_ref[p : p + 1, :])
                for p in range(count)
            ],
            -1.0,
            sgn,
        )
        for tile in range(width // 2):
            first, second = items[2 * tile], items[2 * tile + 1]
            real = jnp.where(low, first, swap(second))
            imag = jnp.where(low, swap(first), second)
            for part in range(2):
                to = pl.ds(c * SUB * pitch + 2 * tile + part, SUB, stride=pitch)
                by_real[to, :] = real
                by_imag[to, :] = imag

    def mix(c, size):
        def body(q, carry):
            def spot(index):
                return pl.ds(pl.multiple_of(index * pitch + q * SUB, SUB), SUB)

            with_real = [
                jnp.where(odd, by_imag[spot(c * SUB + g), :], by_real[spot(c * SUB + g), :])
                for g in range(size)
            ]
            with_imag = [jnp.zeros((SUB, LANES), jnp.float32) for _ in range(size)]
            for m in range(modes):
                real, imag = by_real[spot(m), :], by_imag[spot(m), :]
                for g in range(size):
                    factor = c_ref[c * SUB + g, m, tile_rows(q), :]
                    with_real[g] = with_real[g] + factor * real
                    with_imag[g] = with_imag[g] + factor * imag
            for g in range(size):
                other = jnp.where(
                    odd, pltpu.roll(with_imag[g], 1, 0), -pltpu.roll(with_imag[g], SUB - 1, 0)
                )
                total[spot(g), :] = with_real[g] + other
            return carry

        lax.fori_loop(0, width // SUB, body, 0)

    def row_out(dst, ex, c):
        at = tile_rows(c)
        if modes % SUB == 0:
            mix(c, SUB)
        else:
            pl.when(c < chunks - 1)(lambda: mix(c, SUB))
            pl.when(c == chunks - 1)(lambda: mix(c, modes % SUB))
        items = []
        for tile in range(width // 2):
            lanes = pl.ds(tile * LANES, LANES)
            real, imag = rotate(
                total[pl.ds(2 * tile, SUB, stride=pitch), :],
                total[pl.ds(2 * tile + 1, SUB, stride=pitch), :],
                spread_cos_ref[at, lanes],
                spread_sin_ref[at, lanes],
            )
            items.append(jnp.where(low, real, swap(imag)))
            items.append(jnp.where(low, swap(real), imag))
        for p, value in enumerate(short_fft(items, 1.0, sgn)):
            spec[p] = packed_mul(value, tw_cos_ref[p : p + 1, :], -tw_sin_ref[p : p + 1, :])
        block = spec[...].reshape(count * SUB, LANES)
        dst[:, at, :] = long_dft(block, inv_ref[...]).reshape(count, SUB, LANES)
        post(block_of(dst), ex, c, 0)

    def columns_in(ex, c):
        at = tile_rows(c)
        items = [
            packed_mul(
                recv[ex, d, at, :],
                twist_cos_ref[d : d + 1, :],
                -twist_sin_ref[d : d + 1, :],
            )
            for d in range(count)
        ]
        for a, value in enumerate(short_fft(items, 1.0, sgn)):
            field[a, at, :] = value
            acc[a] = acc[a] + value * value

    def power():
        def body(k, carry):
            at = pl.ds(k * SUB, SUB)
            part = jnp.sum(acc[at], axis=1, keepdims=True)
            acc[at] = jnp.broadcast_to(2.0 * (part + swap(part)), (SUB, SUB, LANES))
            return carry

        lax.fori_loop(0, count // SUB, body, 0)

    def kerr(target, c, to):
        at = tile_rows(c)
        gain = gain_ref[at, :]

        half = SUB // 2
        for k in range(count // SUB):
            first, second = pl.ds(k * SUB, half), pl.ds(k * SUB + half, half)
            values, angles = [], []
            for part in (first, second):
                x = field[part, at, :]
                square = x * x
                values.append(x)
                angles.append(acc[part] - (square + swap(square)))
            sine, cosine = sine_cosine(gain * jnp.where(low, angles[0], angles[1]))
            other_sine, other_cosine = swap(sine), swap(cosine)
            pairs = (
                (jnp.where(low, cosine, other_cosine), jnp.where(low, -sine, other_sine)),
                (jnp.where(low, other_cosine, cosine), jnp.where(low, -other_sine, sine)),
            )
            for part, x, (cosines, sines) in zip((first, second), values, pairs):
                target[part, to, :] = packed_mul(x, cosines, sines)

    ex = 1
    for repeat in range(STEPS):
        dst = send.at[ex - 1]
        if repeat == 0:

            def begin(c):
                arrive(0, c)
                columns_out(recv.at[0], tile_rows(c), dst, ex, c)

            each(begin)
            post_rest(block_of(dst), ex)
        else:
            power()

            def bend(c):
                kerr(spec, c, pl.ds(0, SUB))
                columns_out(spec, pl.ds(0, SUB), dst, ex, c)

            each(bend)
            post_rest(block_of(dst), ex)

        def inward(c):
            arrive(ex, c)
            row_in(ex, c)

        each(inward)
        if repeat == 0:
            load.wait()
        ex += 1
        each(lambda c: row_out(send.at[ex - 1], ex, c))
        post_rest(block_of(send.at[ex - 1]), ex)
        acc[...] = jnp.zeros_like(acc)

        def collect(c):
            arrive(ex, c)
            columns_in(ex, c)

        each(collect)
        ex += 1
    power()

    def finish(c):
        kerr(send.at[ex - 1], c, tile_rows(c))
        post(block_of(send.at[ex - 1]), ex, c, 0)

    each(finish)
    post_rest(block_of(send.at[ex - 1]), ex)

    for c in range(chunks):
        arrive(ex, c)
        repack(2 * c)
        if 4 * (2 * c + 1) < modes:
            repack(2 * c + 1)
    for ex in range(exchanges):
        sent = send.at[0, pl.ds(0, count - 1), pl.ds(0, modes)]
        remote(sent, sent, ex, 0, (me + 1) % count).wait_send()


def mega(pulses, coupling, terms, gain, tw_cos, tw_sin, fwd, inv, count, scale):
    modes, width = coupling.shape[0], coupling.shape[2]
    rows = -(-modes // SUB) * SUB
    pitch = width + SUB
    exchanges = 2 * STEPS + 2
    vmem = pl.BlockSpec(memory_space=pltpu.VMEM)
    smem = pl.BlockSpec(memory_space=pltpu.SMEM)
    block = (count, rows, LANES)
    tiles = rows // SUB
    groups = GROUPS if tiles == 4 else (((0, tiles),),) * exchanges
    flat = (count * (rows + SUB), LANES)
    mixed = (rows * pitch, LANES)
    return pl.pallas_call(
        functools.partial(mega_kernel, count, modes, scale, groups),
        out_shape=jax.ShapeDtypeStruct(pulses.shape, pulses.dtype),
        in_specs=[pl.BlockSpec(memory_space=pl.ANY)] * 2 + [smem, smem] + [vmem] * 4,
        out_specs=vmem,
        scratch_shapes=[
            pltpu.VMEM(pulses.shape, jnp.float32),
            pltpu.VMEM(coupling.shape, jnp.float32),
            pltpu.VMEM(flat, jnp.float32),
            pltpu.VMEM((exchanges - 1,) + block, jnp.float32),
            pltpu.VMEM(flat, jnp.float32),
            pltpu.VMEM((exchanges - 1,) + block, jnp.float32),
            pltpu.VMEM((count, SUB, LANES), jnp.float32),
            pltpu.VMEM(mixed, jnp.float32),
            pltpu.VMEM(mixed, jnp.float32),
            pltpu.VMEM((SUB * pitch, LANES), jnp.float32),
            pltpu.VMEM(block, jnp.float32),
            pltpu.VMEM((count, SUB, LANES), jnp.float32),
            pltpu.VMEM((rows, width // 2 * LANES), jnp.float32),
            pltpu.VMEM((rows, width // 2 * LANES), jnp.float32),
            pltpu.VMEM((count, LANES), jnp.float32),
            pltpu.VMEM((count, LANES), jnp.float32),
            pltpu.VMEM((rows, LANES), jnp.float32),
            pltpu.SemaphoreType.DMA((exchanges,)),
            pltpu.SemaphoreType.DMA((exchanges, tiles)),
            pltpu.SemaphoreType.DMA((2,)),
        ],
        compiler_params=pltpu.CompilerParams(collective_id=0, has_side_effects=True),
        name="mega",
    )(pulses, coupling, terms, gain, tw_cos, tw_sin, fwd, inv)


def packed_table(cosine, sine):
    xp = np if isinstance(cosine, np.ndarray) else jnp
    return (
        xp.concatenate((cosine, cosine), axis=1).astype(xp.float32),
        xp.concatenate((-sine, sine), axis=1).astype(xp.float32),
    )


def lane_order(size):
    place = np.arange(size)
    return place % ROW * (size // ROW) + place // ROW


def dft_weights(size, orient, scale):
    first, second = lane_order(size), np.arange(size)
    if orient > 0:
        first, second = second, first
    angle = orient * 2.0 * np.pi * (first[:, None] * second[None, :] % size) / size
    cosine, sine = scale * np.cos(angle), scale * np.sin(angle)
    full = np.block([[cosine, sine], [-sine, cosine]]).astype(np.float32)
    high = full.astype(jnp.bfloat16)
    low = (full - high.astype(np.float32)).astype(jnp.bfloat16)
    return np.block([[high, low], [high, np.zeros_like(low)]])


def packed_device(pulses, coupling, dispersion_terms, kerr_gain):
    shards = lax.axis_size("freq")
    modes, local = pulses.shape[2], pulses.shape[3]
    groups = local // shards
    tiles = local // LANES
    scale = 1.0 / (local * shards)

    shard_index = np.arange(shards)
    angle = -2.0 * np.pi * (shard_index[:, None] * np.arange(groups)[None, :] % local) / local
    tw_cos, tw_sin = packed_table(np.cos(angle), np.sin(angle))
    fwd, inv = dft_weights(groups, -1.0, 1.0), dft_weights(groups, 1.0, scale)
    coupling = coupling.reshape(2, modes, modes, tiles, LANES).transpose(1, 2, 3, 0, 4)
    coupling = coupling.reshape(modes, modes, 2 * tiles, LANES)
    x = pulses.reshape(2, modes, tiles, LANES).transpose(1, 2, 0, 3).reshape(modes, 2 * tiles, LANES)
    x = mega(x, coupling, dispersion_terms, kerr_gain, tw_cos, tw_sin, fwd, inv, shards, scale)
    x = x.reshape(modes, tiles, 2, LANES).transpose(2, 0, 1, 3)
    return x.reshape(1, 2, modes, local)


def fits(shards, pulses):
    local = pulses.shape[3] // shards
    return (
        pulses.shape[0] == 1
        and shards & (shards - 1) == 0
        and shards == 2 * ROW
        and local == shards * HALF
    )


def solution(mesh):
    in_specs = (P(None, None, None, "freq"), P(None, None, None, "freq"), P(), P())
    out_specs = P(None, None, None, "freq")
    shards = mesh.shape["freq"]

    def run(pulses, coupling, dispersion_terms, kerr_gain):
        body = packed_device if fits(shards, pulses) else per_device
        return jax.shard_map(
            body, mesh=mesh, in_specs=in_specs, out_specs=out_specs, check_vma=False
        )(pulses, coupling, dispersion_terms, kerr_gain)

    return run
```

```python
import functools

import jax
import jax.numpy as jnp
import numpy as np
from jax import lax
from jax.experimental import pallas as pl
from jax.experimental.pallas import tpu as pltpu
from jax.sharding import PartitionSpec as P

STEPS = 2


HIGHEST = lax.Precision.HIGHEST


def angle_table(first, second, modulus, orient):
    turns = first[:, None] * second[None, :] % modulus
    radians = turns.astype(jnp.float32) * (2.0 * jnp.pi / modulus)
    return (jnp.cos(radians), orient * jnp.sin(radians))


def rotate(real_part, imag_part, cosine, sine):
    return (real_part * cosine - imag_part * sine, real_part * sine + imag_part * cosine)


def transform(stacked, cosine, sine):
    real_part = stacked[:, 0]
    imag_part = stacked[:, 1]
    out_real = jnp.matmul(real_part, cosine, precision=HIGHEST) - jnp.matmul(
        imag_part, sine, precision=HIGHEST
    )
    out_imag = jnp.matmul(real_part, sine, precision=HIGHEST) + jnp.matmul(
        imag_part, cosine, precision=HIGHEST
    )
    return jnp.stack((out_real, out_imag), axis=1)


def nonlinear_phase(stacked, kerr_gain):
    magnitude = stacked[:, 0] ** 2 + stacked[:, 1] ** 2
    total_power = jnp.sum(magnitude, axis=1, keepdims=True)
    gains = kerr_gain.reshape((1, -1) + (1,) * (magnitude.ndim - 2))
    angles = gains * (2.0 * total_power - magnitude)
    real_part, imag_part = rotate(stacked[:, 0], stacked[:, 1], jnp.cos(angles), jnp.sin(angles))
    return jnp.stack((real_part, imag_part), axis=1)


def per_device(pulses, coupling, dispersion_terms, kerr_gain):
    shards = lax.axis_size("freq")
    device = lax.axis_index("freq")
    mode_count = pulses.shape[2]
    local_count = pulses.shape[3]
    groups = local_count // shards
    total_count = local_count * shards
    column_index = jnp.arange(shards, dtype=jnp.int32)
    row_index = jnp.arange(local_count, dtype=jnp.int32)
    short_cos, short_sin = angle_table(column_index, column_index, shards, -1.0)
    inverse_short_cos, inverse_short_sin = angle_table(column_index, column_index, shards, 1.0)
    long_cos, long_sin = angle_table(row_index, row_index, local_count, -1.0)
    inverse_long_cos, inverse_long_sin = angle_table(row_index, row_index, local_count, 1.0)
    sample_rows = jnp.arange(groups, dtype=jnp.int32) * shards + device
    twist_cos, twist_sin = angle_table(sample_rows, column_index, total_count, -1.0)
    untwist_cos, untwist_sin = angle_table(row_index, jnp.reshape(device, (1,)), total_count, 1.0)
    untwist_cos = untwist_cos.reshape(-1)
    untwist_sin = untwist_sin.reshape(-1)
    bins = device + shards * row_index
    signed_bin = jnp.where(bins < total_count // 2, bins, bins - total_count).astype(jnp.float32)
    angular = signed_bin / (total_count // 2)
    dispersion = (
        dispersion_terms[0][:, None] * angular
        + dispersion_terms[1][:, None] * angular**2 / 2
        + dispersion_terms[2][:, None] * angular**3 / 6
    )
    spread_cos = jnp.cos(dispersion)
    spread_sin = jnp.sin(dispersion)
    identity = jnp.eye(mode_count, dtype=jnp.float32)[:, :, None]
    mixing_real = coupling[0] + identity
    mixing_imag = coupling[1]
    blocks = pulses.reshape(pulses.shape[0], 2, mode_count, groups, shards)
    columns = lax.all_to_all(blocks, "freq", split_axis=4, concat_axis=4, tiled=True)
    for repeat in range(STEPS):
        spectral = transform(columns, short_cos, short_sin)
        forward_real_part, forward_imag_part = rotate(
            spectral[:, 0], spectral[:, 1], twist_cos, twist_sin
        )
        evolve_rows = lax.all_to_all(
            jnp.stack((forward_real_part, forward_imag_part), axis=1),
            "freq",
            split_axis=4,
            concat_axis=4,
            tiled=True,
        )
        flat = evolve_rows.reshape(evolve_rows.shape[0], 2, mode_count, local_count)
        spectrum = transform(flat, long_cos, long_sin)
        spec_real = spectrum[:, 0]
        spec_imag = spectrum[:, 1]
        mixed_real = jnp.einsum(
            "nmk,bmk->bnk", mixing_real, spec_real, precision=HIGHEST
        ) - jnp.einsum("nmk,bmk->bnk", mixing_imag, spec_imag, precision=HIGHEST)
        mixed_imag = jnp.einsum(
            "nmk,bmk->bnk", mixing_real, spec_imag, precision=HIGHEST
        ) + jnp.einsum("nmk,bmk->bnk", mixing_imag, spec_real, precision=HIGHEST)
        real_part, imag_part = rotate(mixed_real, mixed_imag, spread_cos, spread_sin)
        inverted = transform(
            jnp.stack((real_part, imag_part), axis=1), inverse_long_cos, inverse_long_sin
        )
        real_part, imag_part = rotate(inverted[:, 0], inverted[:, 1], untwist_cos, untwist_sin)
        moved = jnp.stack((real_part, imag_part), axis=1).reshape(evolve_rows.shape)
        columns = nonlinear_phase(
            transform(
                lax.all_to_all(moved, "freq", split_axis=4, concat_axis=4, tiled=True),
                inverse_short_cos,
                inverse_short_sin,
            )
            * (1.0 / total_count),
            kerr_gain,
        )
    returned = lax.all_to_all(columns, "freq", split_axis=4, concat_axis=4, tiled=True)
    return returned.reshape(columns.shape[0], 2, mode_count, local_count)


LANES = 128
HALF = LANES // 2
SUB = 8
ROW = 16
CLASSES = 2
GROUPS = (
    ((0, 2), (2, 4)),
    ((0, 1), (1, 2), (2, 3), (3, 4)),
    ((0, 1), (1, 2), (2, 3), (3, 4)),
    ((0, 1), (1, 2), (2, 3), (3, 4)),
    ((0, 1), (1, 2), (2, 3), (3, 4)),
    ((0, 2), (2, 3), (3, 4)),
)


def low_lanes(shape):
    return lax.broadcasted_iota(jnp.int32, shape, len(shape) - 1) < HALF


def swap(x):
    return pltpu.roll(x, HALF, x.ndim - 1)


def sign_row(rows):
    return jnp.where(low_lanes((rows, LANES)), -1.0, 1.0).astype(jnp.float32)


def times_root(x, index, count, orient, sgn):
    eighth = 8 * index
    if index == 0:
        return x
    if eighth == 2 * count:
        return swap(x) * (sgn * orient)
    angle = 2.0 * np.pi * index / count
    return x * float(np.cos(angle)) + swap(x) * (sgn * float(orient * np.sin(angle)))


def short_fft(items, orient, sgn):
    count = len(items)
    if count == 1:
        return items
    even = short_fft(items[0::2], orient, sgn)
    odd = short_fft(items[1::2], orient, sgn)
    turned = [times_root(v, k, count, orient, sgn) for k, v in enumerate(odd)]
    return [e + t for e, t in zip(even, turned)] + [e - t for e, t in zip(even, turned)]


def packed_mul(x, cosine, signed_sine):
    return x * cosine + swap(x) * signed_sine


def split_constant(value, pieces, bits):
    parts = []
    for _ in range(pieces - 1):
        exponent = np.floor(np.log2(value))
        unit = 2.0 ** (exponent - bits + 1)
        part = np.floor(value / unit) * unit
        parts.append(float(part))
        value -= part
    return parts + [float(value)]


HALF_PI = split_constant(np.pi / 2, 4, 8)


def sine_cosine(theta):
    turns = jnp.floor(theta * float(2 / np.pi) + 0.5)
    rest = theta
    for part in HALF_PI:
        rest = rest - turns * part
    square = rest * rest
    sine = rest + rest * square * (
        -1.6666654611e-1 + square * (8.3321608736e-3 - square * 1.9515295891e-4)
    )
    cosine = 1.0 - 0.5 * square + square * square * (
        4.166664568298827e-2 + square * (-1.388731625493765e-3 + square * 2.443315711809948e-5)
    )
    quadrant = turns.astype(jnp.int32) & 3
    crossed = (quadrant & 1) == 1
    out_sine = jnp.where(crossed, cosine, sine)
    out_cosine = jnp.where(crossed, sine, cosine)
    out_sine = jnp.where(quadrant >= 2, -out_sine, out_sine)
    out_cosine = jnp.where((quadrant == 1) | (quadrant == 2), -out_cosine, out_cosine)
    return out_sine, out_cosine


def long_dft(x, weights):
    high = x.astype(jnp.bfloat16)
    low = (x - high.astype(jnp.float32)).astype(jnp.bfloat16)
    both = jnp.concatenate((high, low), axis=1)
    product = jnp.dot(both, weights, preferred_element_type=jnp.float32)
    return product[:, :LANES] + product[:, LANES:]


def trade(vectors, stride, shift):
    lane = lax.broadcasted_iota(jnp.int32, (SUB, LANES), 1)
    lower = (lane // shift) % 2 == 0
    out = list(vectors)
    for k in range(len(vectors)):
        if (k // stride) % 2 == 0:
            first, second = vectors[k], vectors[k + stride]
            out[k] = jnp.where(lower, first, pltpu.roll(second, shift, 1))
            out[k + stride] = jnp.where(lower, pltpu.roll(first, LANES - shift, 1), second)
    return out


def mega_kernel(
    count, modes, scale, groups, pulse_hbm, c_hbm, terms_ref, gain_in, tw_cos_ref, tw_sin_ref,
    fwd_ref, inv_ref, out_ref, pulse_ref, c_ref, early, recv, late, send, spec, by_real, by_imag, total, field,
    acc, spread_cos_ref, spread_sin_ref, twist_cos_ref, twist_sin_ref, gain_ref,
    send_sem, recv_sem, c_sem,
):
    me = lax.axis_index("freq")
    barrier = pltpu.get_barrier_semaphore()

    def greet(k, carry):
        pl.semaphore_signal(
            barrier, inc=1, device_id=((me + k) % count,), device_id_type=pl.DeviceIdType.MESH
        )
        return carry

    lax.fori_loop(1, count, greet, 0)
    fetch = pltpu.make_async_copy(pulse_hbm, pulse_ref, c_sem.at[0])
    fetch.start()
    load = pltpu.make_async_copy(c_hbm, c_ref, c_sem.at[1])
    load.start()
    chunks = recv.shape[2] // SUB
    rows = recv.shape[2]
    width = c_ref.shape[2]
    pitch = by_real.shape[0] // rows
    span = early.shape[0] // count
    sgn = sign_row(SUB)
    low = low_lanes((SUB, LANES))
    odd = lax.broadcasted_iota(jnp.int32, (SUB, LANES), 0) % 2 == 1
    exchanges = recv.shape[0] + 1

    near = 8
    outer_peers = []
    for k in reversed(range(count // near)):
        place = 0
        for b in range((count // near).bit_length() - 1):
            place = place + ((me // (near << b) + (k >> b)) % 2) * (near << b)
        outer_peers.append(place)
    own_low = me % CLASSES
    step_bits = [(me // (CLASSES << b)) % 2 for b in range((near // CLASSES).bit_length() - 1)]

    def inner_peer(j):
        place = 0
        for b, mine in enumerate(step_bits):
            place = place + ((j // (1 << b) + mine) % 2) * (CLASSES << b)
        return place

    def tile_rows(c):
        return pl.ds(pl.multiple_of(c * SUB, SUB), SUB)

    def block_of(ref):
        return lambda peer, row, size: ref.at[peer, pl.ds(row, size)]

    def flat_of(ref):
        return lambda peer, row, size: ref.at[pl.ds(pl.multiple_of(peer * span + row, SUB), size)]

    def landing(ex):
        return flat_of(late) if ex == exchanges - 1 else block_of(recv.at[ex])

    def remote(src, dst, ex, g, peer):
        return pltpu.make_async_remote_copy(
            src_ref=src,
            dst_ref=dst,
            send_sem=send_sem.at[ex],
            recv_sem=recv_sem.at[ex, g],
            device_id=(peer,),
            device_id_type=pl.DeviceIdType.MESH,
        )

    def extent(ex, g):
        start, end = groups[ex][g]
        return start * SUB, min(end * SUB, modes) - start * SUB

    def post(src, ex, c, kind):
        dst = landing(ex)
        for g, (_, end) in enumerate(groups[ex]):
            row, size = extent(ex, g)

            def go(row=row, size=size, g=g):
                def one(peer):
                    remote(src(peer, row, size), dst(me, row, size), ex, g, peer).start()

                def several(j, carry):
                    inner = inner_peer(near // CLASSES - j)
                    for outer in outer_peers:
                        one(outer + inner + kind)
                    return carry

                lax.fori_loop(1, near // CLASSES, several, 0)
                inner = inner_peer(0)
                for outer in outer_peers[:-1]:
                    one(outer + inner + kind)
                pl.when(own_low != kind)(lambda: one(outer_peers[-1] + inner + kind))

                @pl.when(own_low == kind)
                def _():
                    dst(me, row, size)[...] = src(me, row, size)[...]

            pl.when(c == end - 1)(go)

    def post_rest(src, ex):
        def body(i, carry):
            post(src, ex, i % chunks, 1 + i // chunks)
            return carry

        lax.fori_loop(0, chunks * (CLASSES - 1), body, 0)

    def arrive(ex, c):
        for g, (start, _) in enumerate(groups[ex]):
            row, size = extent(ex, g)

            def go(row=row, size=size, g=g):
                if ex == exchanges - 1:
                    part = late.at[pl.ds(0, (count - 1) * size)]
                else:
                    part = recv.at[ex, pl.ds(0, count - 1), pl.ds(row, size)]
                remote(part, part, ex, g, (me + 1) % count).wait_recv()

            pl.when(c == start)(go)

    def each(body):
        def step(c, carry):
            body(c)
            return carry

        lax.fori_loop(0, chunks, step, 0)

    if rows > modes:
        spare = pl.ds(modes, rows - modes)
        for ex in range(exchanges - 1):
            recv[ex, :, spare, :] = jnp.zeros((count, rows - modes, LANES), jnp.float32)

    def unpack(q):
        names = [min(4 * q + i, modes - 1) for i in range(4)]
        pieces = [
            pulse_ref[m, pl.ds(ri + 2 * SUB * half, SUB, stride=2), :]
            for ri in range(2)
            for m in names
            for half in range(2)
        ]
        turned = jnp.concatenate(pieces, axis=0).T
        for eb in range(count // SUB):
            parts = [turned[gl * count + eb * SUB : gl * count + eb * SUB + SUB] for gl in range(4)]
            parts = trade(trade(parts, 2, 2 * ROW), 1, ROW)
            for i in range(4):
                if 4 * q + i < modes:
                    early[pl.ds(eb * SUB * span + 4 * q + i, SUB, stride=span), :] = parts[i]

    def repack(q):
        names = [min(4 * q + i, modes - 1) for i in range(4)]
        pieces = [[] for _ in range(4)]
        for eb in range(count // SUB):
            parts = [late[pl.ds(eb * SUB * span + m, SUB, stride=span), :] for m in names]
            parts = trade(trade(parts, 1, ROW), 2, 2 * ROW)
            for gl in range(4):
                pieces[gl].append(parts[gl])
        turned = jnp.concatenate([p for piece in pieces for p in piece], axis=0).T
        for ri in range(2):
            for i in range(4):
                if 4 * q + i < modes:
                    for half in range(2):
                        at = (ri * 4 + i) * ROW + half * SUB
                        out_ref[4 * q + i, pl.ds(ri + 2 * SUB * half, SUB, stride=2), :] = turned[
                            at : at + SUB
                        ]

    fetch.wait()
    for q in range(-(-modes // 4)):
        unpack(q)
    pl.semaphore_wait(barrier, count - 1)
    each(lambda c: post(flat_of(early), 0, c, 0))
    post_rest(flat_of(early), 0)

    lane = lax.broadcasted_iota(jnp.int32, (SUB, LANES), 1)
    line = lax.broadcasted_iota(jnp.int32, (SUB, LANES), 0)
    place = lane % HALF
    sample = me + count * (place % ROW * 4 + place // ROW)
    total_count = count * count * HALF
    for c in range(count // SUB):
        turns = (line + c * SUB) * sample
        sine, cosine = sine_cosine(turns.astype(jnp.float32) * (2.0 * np.pi / total_count))
        twist_cos_ref[tile_rows(c), :] = cosine
        twist_sin_ref[tile_rows(c), :] = sine * -sgn

    def by_mode(read, c):
        value = jnp.zeros((SUB, LANES), jnp.float32)
        for r in range(min(SUB, modes - c * SUB)):
            value = jnp.where(line == r, read(c * SUB + r), value)
        return value

    for c in range(chunks):
        gain_ref[tile_rows(c), :] = by_mode(lambda m: gain_in[m], c)
        factors = [by_mode(lambda m: terms_ref[k, m], c) for k in range(3)]

        def spread(tile, carry):
            bins = me + count * (tile * LANES + lane)
            signed = jnp.where(bins < total_count // 2, bins, bins - total_count)
            angular = signed.astype(jnp.float32) * (2.0 / total_count)
            square = angular * angular
            phase = (
                factors[0] * angular + factors[1] * square / 2 + factors[2] * (square * angular) / 6
            )
            sine, cosine = sine_cosine(phase)
            lanes = pl.ds(pl.multiple_of(tile * LANES, LANES), LANES)
            spread_cos_ref[tile_rows(c), lanes] = cosine
            spread_sin_ref[tile_rows(c), lanes] = sine
            return carry

        lax.fori_loop(0, width // 2, spread, 0, unroll=4)
    total[...] = jnp.zeros_like(total)

    def columns_out(source, where, dst, ex, c):
        at = tile_rows(c)
        items = short_fft([source[a, where, :] for a in range(count)], -1.0, sgn)
        for d, value in enumerate(items):
            dst[d, at, :] = packed_mul(value, twist_cos_ref[d : d + 1, :], twist_sin_ref[d : d + 1, :])
        post(block_of(dst), ex, c, 0)

    def row_in(ex, c):
        at = tile_rows(c)
        block = recv[ex, :, at, :].reshape(count * SUB, LANES)
        spec[...] = long_dft(block, fwd_ref[...]).reshape(count, SUB, LANES)
        items = short_fft(
            [
                packed_mul(spec[p], tw_cos_ref[p : p + 1, :], tw_sin_ref[p : p + 1, :])
                for p in range(count)
            ],
            -1.0,
            sgn,
        )
        for tile in range(width // 2):
            first, second = items[2 * tile], items[2 * tile + 1]
            real = jnp.where(low, first, swap(second))
            imag = jnp.where(low, swap(first), second)
            for part in range(2):
                to = pl.ds(c * SUB * pitch + 2 * tile + part, SUB, stride=pitch)
                by_real[to, :] = real
                by_imag[to, :] = imag

    def mix(c, size):
        def body(q, carry):
            def spot(index):
                return pl.ds(pl.multiple_of(index * pitch + q * SUB, SUB), SUB)

            with_real = [
                jnp.where(odd, by_imag[spot(c * SUB + g), :], by_real[spot(c * SUB + g), :])
                for g in range(size)
            ]
            with_imag = [jnp.zeros((SUB, LANES), jnp.float32) for _ in range(size)]
            for m in range(modes):
                real, imag = by_real[spot(m), :], by_imag[spot(m), :]
                for g in range(size):
                    factor = c_ref[c * SUB + g, m, tile_rows(q), :]
                    with_real[g] = with_real[g] + factor * real
                    with_imag[g] = with_imag[g] + factor * imag
            for g in range(size):
                other = jnp.where(
                    odd, pltpu.roll(with_imag[g], 1, 0), -pltpu.roll(with_imag[g], SUB - 1, 0)
                )
                total[spot(g), :] = with_real[g] + other
            return carry

        lax.fori_loop(0, width // SUB, body, 0)

    def row_out(dst, ex, c):
        at = tile_rows(c)
        if modes % SUB == 0:
            mix(c, SUB)
        else:
            pl.when(c < chunks - 1)(lambda: mix(c, SUB))
            pl.when(c == chunks - 1)(lambda: mix(c, modes % SUB))
        items = []
        for tile in range(width // 2):
            lanes = pl.ds(tile * LANES, LANES)
            real, imag = rotate(
                total[pl.ds(2 * tile, SUB, stride=pitch), :],
                total[pl.ds(2 * tile + 1, SUB, stride=pitch), :],
                spread_cos_ref[at, lanes],
                spread_sin_ref[at, lanes],
            )
            items.append(jnp.where(low, real, swap(imag)))
            items.append(jnp.where(low, swap(real), imag))
        for p, value in enumerate(short_fft(items, 1.0, sgn)):
            spec[p] = packed_mul(value, tw_cos_ref[p : p + 1, :], -tw_sin_ref[p : p + 1, :])
        block = spec[...].reshape(count * SUB, LANES)
        dst[:, at, :] = long_dft(block, inv_ref[...]).reshape(count, SUB, LANES)
        post(block_of(dst), ex, c, 0)

    def columns_in(ex, c):
        at = tile_rows(c)
        items = [
            packed_mul(
                recv[ex, d, at, :],
                twist_cos_ref[d : d + 1, :],
                -twist_sin_ref[d : d + 1, :],
            )
            for d in range(count)
        ]
        for a, value in enumerate(short_fft(items, 1.0, sgn)):
            field[a, at, :] = value
            acc[a] = acc[a] + value * value

    def power():
        def body(k, carry):
            at = pl.ds(k * SUB, SUB)
            part = jnp.sum(acc[at], axis=1, keepdims=True)
            acc[at] = jnp.broadcast_to(2.0 * (part + swap(part)), (SUB, SUB, LANES))
            return carry

        lax.fori_loop(0, count // SUB, body, 0)

    def kerr(target, c, to):
        at = tile_rows(c)
        gain = gain_ref[at, :]

        half = SUB // 2
        for k in range(count // SUB):
            first, second = pl.ds(k * SUB, half), pl.ds(k * SUB + half, half)
            values, angles = [], []
            for part in (first, second):
                x = field[part, at, :]
                square = x * x
                values.append(x)
                angles.append(acc[part] - (square + swap(square)))
            sine, cosine = sine_cosine(gain * jnp.where(low, angles[0], angles[1]))
            other_sine, other_cosine = swap(sine), swap(cosine)
            pairs = (
                (jnp.where(low, cosine, other_cosine), jnp.where(low, -sine, other_sine)),
                (jnp.where(low, other_cosine, cosine), jnp.where(low, -other_sine, sine)),
            )
            for part, x, (cosines, sines) in zip((first, second), values, pairs):
                target[part, to, :] = packed_mul(x, cosines, sines)

    ex = 1
    for repeat in range(STEPS):
        dst = send.at[ex - 1]
        if repeat == 0:

            def begin(c):
                arrive(0, c)
                columns_out(recv.at[0], tile_rows(c), dst, ex, c)

            each(begin)
            post_rest(block_of(dst), ex)
        else:
            power()

            def bend(c):
                kerr(spec, c, pl.ds(0, SUB))
                columns_out(spec, pl.ds(0, SUB), dst, ex, c)

            each(bend)
            post_rest(block_of(dst), ex)

        def inward(c):
            arrive(ex, c)
            row_in(ex, c)

        each(inward)
        if repeat == 0:
            load.wait()
        ex += 1
        each(lambda c: row_out(send.at[ex - 1], ex, c))
        post_rest(block_of(send.at[ex - 1]), ex)
        acc[...] = jnp.zeros_like(acc)

        def collect(c):
            arrive(ex, c)
            columns_in(ex, c)

        each(collect)
        ex += 1
    power()

    def finish(c):
        kerr(send.at[ex - 1], c, tile_rows(c))
        post(block_of(send.at[ex - 1]), ex, c, 0)

    each(finish)
    post_rest(block_of(send.at[ex - 1]), ex)

    for c in range(chunks):
        arrive(ex, c)
        repack(2 * c)
        if 4 * (2 * c + 1) < modes:
            repack(2 * c + 1)
    for ex in range(exchanges):
        sent = send.at[0, pl.ds(0, count - 1), pl.ds(0, modes)]
        remote(sent, sent, ex, 0, (me + 1) % count).wait_send()


def mega(pulses, coupling, terms, gain, tw_cos, tw_sin, fwd, inv, count, scale):
    modes, width = coupling.shape[0], coupling.shape[2]
    rows = -(-modes // SUB) * SUB
    pitch = width + SUB
    exchanges = 2 * STEPS + 2
    vmem = pl.BlockSpec(memory_space=pltpu.VMEM)
    smem = pl.BlockSpec(memory_space=pltpu.SMEM)
    block = (count, rows, LANES)
    tiles = rows // SUB
    groups = GROUPS if tiles == 4 else (((0, tiles),),) * exchanges
    flat = (count * (rows + SUB), LANES)
    mixed = (rows * pitch, LANES)
    return pl.pallas_call(
        functools.partial(mega_kernel, count, modes, scale, groups),
        out_shape=jax.ShapeDtypeStruct(pulses.shape, pulses.dtype),
        in_specs=[pl.BlockSpec(memory_space=pl.ANY)] * 2 + [smem, smem] + [vmem] * 4,
        out_specs=vmem,
        scratch_shapes=[
            pltpu.VMEM(pulses.shape, jnp.float32),
            pltpu.VMEM(coupling.shape, jnp.float32),
            pltpu.VMEM(flat, jnp.float32),
            pltpu.VMEM((exchanges - 1,) + block, jnp.float32),
            pltpu.VMEM(flat, jnp.float32),
            pltpu.VMEM((exchanges - 1,) + block, jnp.float32),
            pltpu.VMEM((count, SUB, LANES), jnp.float32),
            pltpu.VMEM(mixed, jnp.float32),
            pltpu.VMEM(mixed, jnp.float32),
            pltpu.VMEM((SUB * pitch, LANES), jnp.float32),
            pltpu.VMEM(block, jnp.float32),
            pltpu.VMEM((count, SUB, LANES), jnp.float32),
            pltpu.VMEM((rows, width // 2 * LANES), jnp.float32),
            pltpu.VMEM((rows, width // 2 * LANES), jnp.float32),
            pltpu.VMEM((count, LANES), jnp.float32),
            pltpu.VMEM((count, LANES), jnp.float32),
            pltpu.VMEM((rows, LANES), jnp.float32),
            pltpu.SemaphoreType.DMA((exchanges,)),
            pltpu.SemaphoreType.DMA((exchanges, tiles)),
            pltpu.SemaphoreType.DMA((2,)),
        ],
        compiler_params=pltpu.CompilerParams(collective_id=0, has_side_effects=True),
        name="mega",
    )(pulses, coupling, terms, gain, tw_cos, tw_sin, fwd, inv)


def packed_table(cosine, sine):
    xp = np if isinstance(cosine, np.ndarray) else jnp
    return (
        xp.concatenate((cosine, cosine), axis=1).astype(xp.float32),
        xp.concatenate((-sine, sine), axis=1).astype(xp.float32),
    )


def lane_order(size):
    place = np.arange(size)
    return place % ROW * (size // ROW) + place // ROW


def dft_weights(size, orient, scale):
    first, second = lane_order(size), np.arange(size)
    if orient > 0:
        first, second = second, first
    angle = orient * 2.0 * np.pi * (first[:, None] * second[None, :] % size) / size
    cosine, sine = scale * np.cos(angle), scale * np.sin(angle)
    full = np.block([[cosine, sine], [-sine, cosine]]).astype(np.float32)
    high = full.astype(jnp.bfloat16)
    low = (full - high.astype(np.float32)).astype(jnp.bfloat16)
    return np.block([[high, low], [high, np.zeros_like(low)]])


def packed_device(pulses, coupling, dispersion_terms, kerr_gain):
    shards = lax.axis_size("freq")
    modes, local = pulses.shape[2], pulses.shape[3]
    groups = local // shards
    tiles = local // LANES
    scale = 1.0 / (local * shards)

    shard_index = np.arange(shards)
    angle = -2.0 * np.pi * (shard_index[:, None] * np.arange(groups)[None, :] % local) / local
    tw_cos, tw_sin = packed_table(np.cos(angle), np.sin(angle))
    fwd, inv = dft_weights(groups, -1.0, 1.0), dft_weights(groups, 1.0, scale)
    coupling = coupling.reshape(2, modes, modes, tiles, LANES).transpose(1, 2, 3, 0, 4)
    coupling = coupling.reshape(modes, modes, 2 * tiles, LANES)
    x = pulses.reshape(2, modes, tiles, LANES).transpose(1, 2, 0, 3).reshape(modes, 2 * tiles, LANES)
    x = mega(x, coupling, dispersion_terms, kerr_gain, tw_cos, tw_sin, fwd, inv, shards, scale)
    x = x.reshape(modes, tiles, 2, LANES).transpose(2, 0, 1, 3)
    return x.reshape(1, 2, modes, local)


def fits(shards, pulses):
    local = pulses.shape[3] // shards
    return (
        pulses.shape[0] == 1
        and shards & (shards - 1) == 0
        and shards == 2 * ROW
        and local == shards * HALF
    )


def solution(mesh):
    in_specs = (P(None, None, None, "freq"), P(None, None, None, "freq"), P(), P())
    out_specs = P(None, None, None, "freq")
    shards = mesh.shape["freq"]

    def run(pulses, coupling, dispersion_terms, kerr_gain):
        body = packed_device if fits(shards, pulses) else per_device
        return jax.shard_map(
            body, mesh=mesh, in_specs=in_specs, out_specs=out_specs, check_vma=False
        )(pulses, coupling, dispersion_terms, kerr_gain)

    return run
```
